8 devices in a mesh: spin: 1 (over z), row: 2 (over y), col: 4 (over x, core).
Axes of the slice: x: 2, y: 2, z: 1, core: 2. Of those that a mesh axis runs over, the one named last changes fastest.
Arguments:
- hamiltonian: float32 [2048, 2048], P(('spin', 'row'), 'col')
- bounds: float32 [2], P('spin')
- n_occ: int32 [1], P('spin')
Outputs:
- output 1: float32 [2048, 2048], P(('spin', 'row'), 'col')
- output 2: float32 [1], P('spin')
All inputs are finite; a program needn't handle non-finite values.
Results may differ from the reference program's by a relative error of at most 0.001.
Values sent between devices are 32-bit elements.
A program may use at most 1 GiB of HBM per device.

```python
import jax
import jax.numpy as jnp
from jax import lax

N = 2048
STEPS = 3


def setup_inputs(seed: int = 0, part: int = 0) -> dict:
    key = jax.random.fold_in(jax.random.key(seed), part)
    k_off, k_diag, k_shift, k_margin, k_occ = jax.random.split(key, 5)
    gauss_mat = jax.random.normal(k_off, (N, N), jnp.float32)
    sym_part = (gauss_mat + gauss_mat.T) * (2.0 * N) ** -0.5
    unif_diag = jax.random.uniform(k_diag, (N,), jnp.float32)
    shift_val = 2.0 + jax.random.uniform(k_shift, (), jnp.float32)
    diag_vals = shift_val + 0.8 * (3.0 * unif_diag * unif_diag - 1.0)
    index_vec = jnp.arange(N)
    on_diag = index_vec[:, None] == index_vec[None, :]
    hamiltonian = jnp.where(on_diag, diag_vals[None, :], sym_part)
    margins = jax.random.uniform(k_margin, (2,), jnp.float32, 0.0, 0.5)
    bounds = jnp.stack([jnp.min(diag_vals) - 2.4 - margins[0], jnp.max(diag_vals) + 2.4 + margins[1]])
    n_occ = jax.random.randint(k_occ, (1,), 3 * N // 20, 7 * N // 20 + 1, jnp.int32)
    return {"hamiltonian": hamiltonian, "bounds": bounds, "n_occ": n_occ}


def reference(hamiltonian, bounds, n_occ):
    occupied = n_occ[0].astype(jnp.float32)
    mu_val = jnp.trace(hamiltonian) / N
    lam_scale = jnp.minimum(occupied / (bounds[1] - mu_val), (N - occupied) / (mu_val - bounds[0]))
    identity = jnp.eye(N, dtype=jnp.float32)
    density = (lam_scale / N) * (mu_val * identity - hamiltonian) + (occupied / N) * identity

    def purify_step(dens_cur, unused_x):
        dens_sq = jnp.dot(dens_cur, dens_cur, preferred_element_type=jnp.float32, precision=lax.Precision.HIGHEST)
        dens_cube = jnp.dot(dens_sq, dens_cur, preferred_element_type=jnp.float32, precision=lax.Precision.HIGHEST)
        trace_x = jnp.trace(dens_cur)
        trace_sq = jnp.sum(dens_cur * dens_cur)
        trace_cube = jnp.sum(dens_sq * dens_cur)
        mix_coef = (trace_sq - trace_cube) / (trace_x - trace_sq)
        updated = ((1.0 - 2.0 * mix_coef) * dens_cur + (1.0 + mix_coef) * dens_sq - dens_cube) / (1.0 - mix_coef)
        return updated, None

    density, _ = lax.scan(purify_step, density, None, length=STEPS)
    energy = 2.0 * jnp.sum(density * hamiltonian)
    return density, energy[None]
```

```python
import jax
import jax.numpy as jnp
from jax import lax
from jax.experimental import pallas as pl
from jax.experimental.pallas import tpu as pltpu
from jax.sharding import PartitionSpec as P

STEPS = 3
PANELS = 8
SLOTS = 5
MESH = pl.DeviceIdType.MESH
NN = (((1,), (0,)), ((), ()))
NT = (((1,), (1,)), ((), ()))


def dot(lhs, rhs, dims):
    return lax.dot_general(lhs, rhs, dims, precision=lax.Precision.HIGHEST, preferred_element_type=jnp.float32)


def pick(index, values):
    return sum(jnp.where(index == k, v, 0) for k, v in enumerate(values))


def flip(bit, by):
    return bit + by - 2 * bit * by


def same(a, b):
    return 1 - (a - b) * (a - b)


def panel_of(x, y, c):
    return 4 * x + 2 * c + y


def h_block(x, y, c, t):
    col_off = t // 2
    row_off = 2 * (t % 2) + flip(col_off, y)
    tables = (
        (0, 0, (1, 1, 3, 0, 2), (1, 0, 0, 0, 0)),
        (0, 1, (3, 3, 1, 1, 2), (1, 0, 0, 1, 0)),
        (1, 0, (0, 1, 2, 3, 1), (0, 0, 0, 0, 1)),
        (1, 1, (2, 3, 1, 3, 1), (0, 0, 0, 1, 1)),
    )
    row_on = sum(same(x, tx) * same(c, tc) * pick(t, rows) for tx, tc, rows, _ in tables)
    col_on = sum(same(x, tx) * same(c, tc) * pick(t, cols) for tx, tc, _, cols in tables)
    on = same(x, y)
    return on * row_on + (1 - on) * row_off, on * col_on + (1 - on) * col_off


def kernel(n, bounds, n_occ, h_ref, out_ref, e_ref, buf, hrow, xrow, x2row, acc, parts, coef, sums, send_sem, recv_sem, part_send, part_recv):
    blk_n = n // PANELS
    y = lax.axis_index("row")
    j = lax.axis_index("col")
    x, c = j // 2, j % 2
    me = panel_of(x, y, c)

    def bits(mask):
        return flip(x, mask // 4), flip(y, mask % 2), flip(c, (mask // 2) % 2)

    def device(mask):
        dx, dy, dc = bits(mask)
        return (0, dy, 2 * dx + dc)

    def panel(mask):
        return panel_of(*bits(mask))

    PARTNER, XN, YN, DIAG = 2, 4, 1, 5

    barrier = pltpu.get_barrier_semaphore()
    for mask in range(1, 8):
        pl.semaphore_signal(barrier, inc=1, device_id=device(mask), device_id_type=MESH)
    pl.semaphore_wait(barrier, 7)

    def send(src, buf_id, q, t, way):
        mask = (PARTNER, XN, YN)[way]
        return pltpu.make_async_remote_copy(
            src_ref=src,
            dst_ref=buf.at[buf_id, q, t],
            send_sem=send_sem.at[buf_id, q, t, way],
            recv_sem=recv_sem.at[buf_id, q, t],
            device_id=device(mask),
            device_id_type=MESH,
        )

    def x_first(t, src_y):
        return jnp.where(t == 4, 1 - src_y, 1 - t % 2)

    def forward(buf_id, mask, t, act):
        q = panel(mask)
        block = buf.at[buf_id, q, t]
        if mask in (XN, YN, DIAG):
            act(send(block, buf_id, q, t, 0))
        if mask == XN:

            @pl.when(x_first(t, y) == 1)
            def _():
                act(send(block, buf_id, q, t, 2))

        if mask == YN:

            @pl.when(x_first(t, 1 - y) == 0)
            def _():
                act(send(block, buf_id, q, t, 1))

    def arrive(buf_id, mask, t):
        if mask != 0:
            q = panel(mask)
            send(buf.at[buf_id, q, t], buf_id, q, t, 0).wait_recv()
            forward(buf_id, mask, t, lambda copy: copy.start())

    def drain(buf_id, valid, own_src):
        @pl.loop(0, SLOTS)
        def _(t):
            @pl.when(valid(0, t))
            def _():
                for way in range(3):
                    send(own_src(t), buf_id, me, t, way).wait_send()

            for mask in (XN, YN, DIAG):

                @pl.when(valid(mask, t))
                def _():
                    forward(buf_id, mask, t, lambda copy: copy.wait_send())

    def valid_h(mask, t):
        qx, qy, _ = bits(mask)
        return jnp.logical_or(t < 4, same(qx, qy) == 1)

    def valid_x(mask, t):
        qx, _, qc = bits(mask)
        return jnp.logical_or(t < 4, same(qx, qc) == 1)

    def part_copy(rnd, src, mask):
        return pltpu.make_async_remote_copy(
            src_ref=parts.at[rnd, src],
            dst_ref=parts.at[rnd, src],
            send_sem=part_send.at[rnd, mask],
            recv_sem=part_recv.at[rnd, src],
            device_id=device(mask),
            device_id_type=MESH,
        )

    def sum_start(rnd, vals):
        for k, val in enumerate(vals):
            parts[rnd, me, k] = val
        for mask in range(1, 8):
            part_copy(rnd, me, mask).start()

    def sum_finish(rnd, count):
        for mask in range(1, 8):
            part_copy(rnd, panel(mask), mask).wait_recv()
        for mask in range(1, 8):
            part_copy(rnd, me, mask).wait_send()
        out = []
        for k in range(count):
            tot = parts[rnd, 0, k]
            for q in range(1, PANELS):
                tot = tot + parts[rnd, q, k]
            out.append(jnp.sum(jnp.sum(tot, axis=1, keepdims=True), axis=0, keepdims=True))
        return out

    def fold(val):
        rows, cols = val.shape
        val = jnp.sum(val.reshape(rows // 8, 8, cols), axis=0)
        tot = val[:, :128]
        for k in range(1, cols // 128):
            tot = tot + val[:, k * 128 : (k + 1) * 128]
        return tot

    def h_src(t):
        a, b = h_block(x, y, c, t)
        return h_ref.at[pl.ds(pl.multiple_of(a * blk_n, blk_n), blk_n), pl.ds(pl.multiple_of(b * blk_n, blk_n), blk_n)]

    HB, LAST = 2, 0

    @pl.loop(0, SLOTS)
    def _(t):
        @pl.when(valid_h(0, t))
        def _():
            for way in range(3):
                send(h_src(t), HB, me, t, way).start()

    rows_n, cols_n = h_ref.shape
    mu_part = jnp.zeros((8, 128), jnp.float32)
    for k in range(rows_n // blk_n):
        tile = h_ref[k * blk_n : (k + 1) * blk_n, :]
        row_ids = y * rows_n + k * blk_n + lax.broadcasted_iota(jnp.int32, tile.shape, 0)
        col_ids = j * cols_n + lax.broadcasted_iota(jnp.int32, tile.shape, 1)
        mu_part = mu_part + fold(jnp.where(row_ids == col_ids, tile, 0.0))
    sum_start(0, [mu_part])

    eye = (lax.broadcasted_iota(jnp.int32, (blk_n, blk_n), 0) == lax.broadcasted_iota(jnp.int32, (blk_n, blk_n), 1)).astype(jnp.float32)
    (trace_h,) = sum_finish(0, 1)
    occ = n_occ[0].astype(jnp.float32)
    mu = trace_h / n
    lam = jnp.minimum(occ / (bounds[1] - mu), (n - occ) / (mu - bounds[0]))
    coef[0:1, :] = jnp.broadcast_to(lam / n, (1, blk_n))
    coef[1:2, :] = jnp.broadcast_to(mu, (1, blk_n))
    coef[2:3, :] = jnp.broadcast_to(jnp.full((1, 1), occ / n, jnp.float32), (1, blk_n))

    def first_x(mask, t):
        qx, qy, qc = bits(mask)
        a, b = h_block(qx, qy, qc, t)
        row, col = 4 * qy + a, 4 * qx + 2 * qc + b
        blk = h_src(t)[...] if mask == 0 else buf[HB, panel(mask), t]
        diag = eye * (row == col).astype(jnp.float32)
        val = coef[0:1, :] * (coef[1:2, :] * diag - blk) + coef[2:3, :] * diag
        diff = (col - row + 8) % 8

        @pl.when(diff <= 4)
        def _():
            buf[0, row, diff] = val

        @pl.when(diff >= 4)
        def _():
            buf[0, col, (8 - diff)] = val.T

        @pl.when(row == me)
        def _():
            hrow[col] = blk
            xrow[col] = val

        @pl.when(jnp.logical_and(col == me, row != me))
        def _():
            hrow[row] = blk.T
            xrow[row] = val.T

    def own_h(src_mask, t):
        return None

    @pl.loop(0, SLOTS)
    def _(t):
        for mask in (0, 2, 4, 1, 6, 3):

            @pl.when(valid_h(mask, t))
            def _():
                arrive(HB, mask, t)
                first_x(mask, t)

    @pl.loop(0, SLOTS)
    def _(t):
        for mask in (5, 7):

            @pl.when(valid_h(mask, t))
            def _():
                arrive(HB, mask, t)
                first_x(mask, t)

    def product(left, b, col):
        tot = dot(left[col], buf[b, col, 0], NN)
        for d in range(1, 4):
            k = (col + 8 - d) % 8
            tot = tot + dot(left[k], buf[b, k, d], NN)
        k = (col + 4) % 8
        tot = tot + dot(left[k], buf[b, k, 4], NN)
        for d in range(1, 4):
            k = (col + d) % 8
            tot = tot + dot(left[k], buf[b, col, d], NT)
        return tot

    @pl.loop(0, PANELS)
    def _(col):
        x2row[col] = product(xrow, 0, col)

    def traces(rnd):
        t1 = fold(xrow[me] * eye)
        sums[...] = jnp.zeros_like(sums)

        @pl.loop(0, PANELS)
        def _(col):
            xv = xrow[col]
            sums[0] += fold(xv * xv)
            sums[1] += fold(xv * x2row[col])

        sum_start(rnd, [t1, sums[0], sums[1]])

    def mix(rnd):
        t1, t2, t3 = sum_finish(rnd, 3)
        cval = (t2 - t3) / (t1 - t2)
        for k, val in enumerate((1.0 - 2.0 * cval, 1.0 + cval, 1.0 - cval)):
            coef[k : k + 1, :] = jnp.broadcast_to(val, (1, blk_n))

    def updated(col):
        return (coef[0:1, :] * xrow[col] + coef[1:2, :] * x2row[col] - acc[...]) / coef[2:3, :]

    for step in range(STEPS - 1):
        old, new = step, step + 1
        traces(1 + step)

        @pl.loop(0, PANELS)
        def _(d):
            col = (me + d) % 8
            acc[...] = product(x2row, old, col)

            @pl.when(d == 0)
            def _():
                if step == 0:
                    drain(HB, valid_h, h_src)
                else:
                    drain(old, valid_x, lambda t: buf.at[old, me, t])
                mix(1 + step)

            val = updated(col)

            @pl.when(d <= 4)
            def _():
                buf[new, me, d] = val

            xrow[col] = val

            @pl.when(jnp.logical_and(d <= 4, valid_x(0, d)))
            def _():
                for way in range(3):
                    send(buf.at[new, me, d], new, me, d, way).start()

        @pl.loop(0, PANELS)
        def _(col):
            x2row[col] = jnp.zeros((blk_n, blk_n), jnp.float32)

        def use(mask, t):
            q = panel(mask)
            col = (q + t) % 8
            blk = buf[new, q, t]
            x2row[col] += dot(xrow[q], blk, NN)

            @pl.when(t > 0)
            def _():
                x2row[q] += dot(xrow[col], blk, NT)

            @pl.when(t == 4)
            def _():
                buf[new, col, 4] = blk.T

        for masks in ((0, 2, 4, 1, 6, 3), (5, 7)):

            @pl.loop(0, SLOTS)
            def _(t):
                for mask in masks:

                    @pl.when(valid_x(mask, t))
                    def _():
                        arrive(new, mask, t)
                        use(mask, t)

    old = STEPS - 1
    traces(STEPS)
    sums[2] = jnp.zeros((8, 128), jnp.float32)

    def last_copy(i):
        return pltpu.make_async_remote_copy(
            src_ref=buf.at[LAST, me, i],
            dst_ref=buf.at[LAST, me, i],
            send_sem=send_sem.at[LAST, me, i, 0],
            recv_sem=recv_sem.at[LAST, me, i],
            device_id=device(YN),
            device_id_type=MESH,
        )

    def place(i, b, val):
        out_ref[pl.ds(pl.multiple_of(i * blk_n, blk_n), blk_n), pl.ds(pl.multiple_of(b * blk_n, blk_n), blk_n)] = val.T

    @pl.loop(0, PANELS)
    def _(d):
        half, i = d // 4, d % 4
        col = 4 * flip(y, 1 - half) + i
        acc[...] = product(x2row, old, col)

        @pl.when(d == 0)
        def _():
            drain(old, valid_x, lambda t: buf.at[old, me, t])
            mix(STEPS)

        val = updated(col)

        @pl.when(half == 0)
        def _():
            buf[LAST, me, i] = val

        sums[2] += fold(val * hrow[col])

        @pl.when(half == 0)
        def _():
            last_copy(i).start()

        @pl.when(half == 1)
        def _():
            place(i, y, val)

    sum_start(STEPS + 1, [sums[2]])

    @pl.loop(0, 4)
    def _(i):
        q = panel(YN)
        pltpu.make_async_remote_copy(
            src_ref=buf.at[LAST, q, i],
            dst_ref=buf.at[LAST, q, i],
            send_sem=send_sem.at[LAST, q, i, 0],
            recv_sem=recv_sem.at[LAST, q, i],
            device_id=device(YN),
            device_id_type=MESH,
        ).wait_recv()
        place(i, 1 - y, buf[LAST, q, i])

    @pl.loop(0, 4)
    def _(i):
        last_copy(i).wait_send()

    (energy,) = sum_finish(STEPS + 1, 1)
    e_ref[0] = 2.0 * jnp.sum(energy)


def solution(mesh):
    n_cols = mesh.shape["col"]

    def local_fn(ham_blk, bounds, n_occ):
        rows_n, cols_n = ham_blk.shape
        n = cols_n * n_cols
        blk_n = n // PANELS
        f32 = jnp.float32
        return pl.pallas_call(
            lambda *refs: kernel(n, *refs),
            out_shape=(jax.ShapeDtypeStruct((rows_n, cols_n), f32), jax.ShapeDtypeStruct((1,), f32)),
            in_specs=[
                pl.BlockSpec(memory_space=pltpu.SMEM),
                pl.BlockSpec(memory_space=pltpu.SMEM),
                pl.BlockSpec(memory_space=pltpu.VMEM),
            ],
            out_specs=(pl.BlockSpec(memory_space=pltpu.VMEM), pl.BlockSpec(memory_space=pltpu.SMEM)),
            scratch_shapes=[
                pltpu.VMEM((3, PANELS, SLOTS, blk_n, blk_n), f32),
                pltpu.VMEM((PANELS, blk_n, blk_n), f32),
                pltpu.VMEM((PANELS, blk_n, blk_n), f32),
                pltpu.VMEM((PANELS, blk_n, blk_n), f32),
                pltpu.VMEM((blk_n, blk_n), f32),
                pltpu.VMEM((STEPS + 2, PANELS, 3, 8, 128), f32),
                pltpu.VMEM((8, blk_n), f32),
                pltpu.VMEM((3, 8, 128), f32),
                pltpu.SemaphoreType.DMA((3, PANELS, SLOTS, 3)),
                pltpu.SemaphoreType.DMA((3, PANELS, SLOTS)),
                pltpu.SemaphoreType.DMA((STEPS + 2, PANELS)),
                pltpu.SemaphoreType.DMA((STEPS + 2, PANELS)),
            ],
            compiler_params=pltpu.CompilerParams(collective_id=0, has_side_effects=True, vmem_limit_bytes=60 << 20),
            name="purify",
        )(bounds, n_occ, ham_blk)

    spec_mat = P(("spin", "row"), "col")
    return jax.shard_map(local_fn, mesh=mesh, in_specs=(spec_mat, P("spin"), P("spin")), out_specs=(spec_mat, P("spin")), check_vma=False)
```

```python
import jax
import jax.numpy as jnp
from jax import lax
from jax.experimental import pallas as pl
from jax.experimental.pallas import tpu as pltpu
from jax.sharding import PartitionSpec as P

STEPS = 3
PANELS = 8
SLOTS = 5
MESH = pl.DeviceIdType.MESH
NN = (((1,), (0,)), ((), ()))
NT = (((1,), (1,)), ((), ()))


def dot(lhs, rhs, dims):
    return lax.dot_general(lhs, rhs, dims, precision=lax.Precision.HIGHEST, preferred_element_type=jnp.float32)


def flag(cond):
    return lax.convert_element_type(cond, jnp.int32)


def pick(index, values):
    return sum(flag(index == k) * v for k, v in enumerate(values) if v)


def half(val, by=2):
    return lax.div(val, jnp.int32(by))


def part(val, by=2):
    return lax.rem(val, jnp.int32(by))


def flip(bit, by):
    return bit + by - 2 * bit * by


def panel_bits(q):
    return q // 4, q % 2, (q // 2) % 2


def packed(digits, base):
    return sum(d * base**k for k, d in enumerate(digits))


def h_blocks(q):
    x, y, c = panel_bits(q)
    if x == y:
        local = {
            (0, 0): ((1, 1), (1, 0), (3, 0), (0, 0), (2, 0)),
            (0, 1): ((3, 1), (3, 0), (1, 0), (1, 1), (2, 0)),
            (1, 0): ((0, 0), (1, 0), (2, 0), (3, 0), (1, 1)),
            (1, 1): ((2, 0), (3, 0), (1, 0), (3, 1), (1, 1)),
        }[x, c]
    else:
        local = tuple((2 * k + (b + y) % 2, b) for b in range(2) for k in range(2))
    return tuple((4 * y + a, 4 * x + 2 * c + b) for a, b in local)


def x_blocks(q):
    x, y, c = panel_bits(q)
    return tuple(q ^ m for m in (4 + 2 * x, 1 + 2 * y, 5 + 2 * y, 0, 2, 7 - 2 * y))


def kernel(n, bounds, n_occ, h_ref, out_ref, e_ref, buf, hrow, x2row, acc, parts, coef, sums, send_sem, recv_sem, part_send, part_recv, last_send, last_recv):
    blk_n = n // PANELS
    y = lax.axis_index("row")
    j = lax.axis_index("col")
    x, c = half(j), part(j)
    me = 4 * x + 2 * c + y
    on = 1 - flip(x, y)

    class Source:
        def __init__(self, q, h_pack, h_count, x_pack, x_count):
            self.fields = q, h_pack, h_count, x_pack, x_count
            self.q, self.h_pack, self.h_count, self.x_pack, self.x_count = self.fields

        def __add__(self, other):
            return Source(*(a + b for a, b in zip(self.fields, other.fields)))

        def __mul__(self, by):
            return Source(*(a * by for a in self.fields))

    def device(mask):
        dx, dy, dc = flip(x, half(mask, 4)), flip(y, part(mask)), flip(c, part(half(mask)))
        return (0, dy, 2 * dx + dc)

    def source(mask):
        q = panel(mask)
        return Source(
            q,
            pick(q, [packed([8 * row + col for row, col in h_blocks(k)], 64) for k in range(PANELS)]),
            pick(q, [len(h_blocks(k)) for k in range(PANELS)]),
            pick(q, [packed(x_blocks(k), 8) for k in range(PANELS)]),
            pick(q, [5 - (k // 2) % 2 for k in range(PANELS)]),
        )

    def panel(mask):
        return 4 * flip(x, mask // 4) + 2 * flip(c, (mask // 2) % 2) + flip(y, mask % 2)

    def h_place(src, t):
        code = part(lax.div(src.h_pack, pick(t, [64**k for k in range(SLOTS)])), 64)
        return half(code, 8), part(code, 8)

    def x_place(src, t):
        return src.q, part(lax.div(src.x_pack, pick(t, [8**k for k in range(SLOTS + 1)])), 8)

    devices = [device(jnp.int32(mask)) for mask in range(8)]
    sources = [source(mask) for mask in range(8)]

    PARTNER, XN, YN, DIAG = 2, 4, 1, 5

    barrier = pltpu.get_barrier_semaphore()
    for mask in range(1, 8):
        pl.semaphore_signal(barrier, inc=1, device_id=devices[mask], device_id_type=MESH)
    pl.semaphore_wait(barrier, 7)

    class Exchange:
        def __init__(self, rnd, buf_id, place, count, own_src=None):
            self.rnd, self.buf_id, self.place, self.count = rnd, buf_id, place, count
            self.own_src = own_src or (lambda row, col: buf.at[buf_id, row, col])

        def copy(self, at, t, way, src=None):
            q, row, col = at
            block = buf.at[self.buf_id, row, col]
            return pltpu.make_async_remote_copy(
                src_ref=block if src is None else src,
                dst_ref=block,
                send_sem=send_sem.at[self.rnd, q, t, way],
                recv_sem=recv_sem.at[self.rnd, q, t],
                device_id=devices[(PARTNER, XN, YN)[way]],
                device_id_type=MESH,
            )

        def own(self, at, t, act):
            for way in range(3):
                act(self.copy(at, t, way, self.own_src(*at[1:])))

        def forward(self, mask, at, t, act):
            if mask in (XN, YN, DIAG):
                act(self.copy(at, t, 0))
            if mask == XN:

                @pl.when(part(t) + flag(t == 4) * y == 0)
                def _():
                    act(self.copy(at, t, 2))

            if mask == YN:

                @pl.when(part(t) + flag(t == 4) * (1 - y) == 1)
                def _():
                    act(self.copy(at, t, 1))

        def arrive(self, mask, at, t):
            self.copy(at, t, 0).wait_recv()
            self.forward(mask, at, t, lambda copy: copy.start())

        def at(self, src, t):
            return (src.q, *self.place(src, t))

        def each(self, jobs, first=0, last=SLOTS):
            @pl.loop(0, last - first)
            def _(i):
                t = i + first
                for mask, body in jobs:
                    src = mask if isinstance(mask, Source) else sources[mask]

                    @pl.when(t < self.count(src))
                    def _():
                        body(mask, self.at(src, t), t)

        def drain(self):
            def fwd(mask, at, t):
                self.forward(mask, at, t, lambda copy: copy.wait_send())

            self.each([(0, lambda mask, at, t: self.own(at, t, lambda copy: copy.wait_send()))] + [(mask, fwd) for mask in (XN, YN, DIAG)])

    def part_copy(rnd, src, mask):
        return pltpu.make_async_remote_copy(
            src_ref=parts.at[rnd, src],
            dst_ref=parts.at[rnd, src],
            send_sem=part_send.at[rnd, mask],
            recv_sem=part_recv.at[rnd, src],
            device_id=devices[mask],
            device_id_type=MESH,
        )

    def sum_start(rnd, vals):
        for k, val in enumerate(vals):
            parts[rnd, me, k] = val
        for mask in range(1, 8):
            part_copy(rnd, me, mask).start()

    def sum_finish(rnd, count):
        for mask in range(1, 8):
            part_copy(rnd, sources[mask].q, mask).wait_recv()
        for mask in range(1, 8):
            part_copy(rnd, me, mask).wait_send()
        out = []
        for k in range(count):
            tot = parts[rnd, 0, k]
            for q in range(1, PANELS):
                tot = tot + parts[rnd, q, k]
            out.append(jnp.sum(jnp.sum(tot, axis=1, keepdims=True), axis=0, keepdims=True))
        return out

    def fold(val):
        rows, cols = val.shape
        val = jnp.sum(val.reshape(rows // 8, 8, cols), axis=0)
        tot = val[:, :128]
        for k in range(1, cols // 128):
            tot = tot + val[:, k * 128 : (k + 1) * 128]
        return tot

    def span(k):
        return pl.ds(pl.multiple_of(k * blk_n, blk_n), blk_n)

    def clear():
        @pl.loop(0, PANELS)
        def _(col):
            x2row[col] = jnp.zeros((blk_n, blk_n), jnp.float32)

    def h_src(row, col):
        return h_ref.at[span(row - 4 * y), span(col - 2 * j)]

    hx = Exchange(0, 1, h_place, lambda src: src.h_count, h_src)
    hx.each([(0, lambda mask, at, t: hx.own(at, t, lambda copy: copy.start()))])

    rows_n, cols_n = h_ref.shape
    mu_part = jnp.zeros((8, 128), jnp.float32)
    for k in range(rows_n // blk_n):
        tile = h_ref[k * blk_n : (k + 1) * blk_n, :]
        row_ids = y * rows_n + k * blk_n + lax.broadcasted_iota(jnp.int32, tile.shape, 0)
        col_ids = j * cols_n + lax.broadcasted_iota(jnp.int32, tile.shape, 1)
        mu_part = mu_part + fold(jnp.where(row_ids == col_ids, tile, 0.0))
    sum_start(0, [mu_part])
    clear()

    eye = (lax.broadcasted_iota(jnp.int32, (blk_n, blk_n), 0) == lax.broadcasted_iota(jnp.int32, (blk_n, blk_n), 1)).astype(jnp.float32)
    (trace_h,) = sum_finish(0, 1)
    occ = n_occ[0].astype(jnp.float32)
    mu = trace_h / n
    lam = jnp.minimum(occ / (bounds[1] - mu), (n - occ) / (mu - bounds[0]))
    coef[0:1, :] = jnp.broadcast_to(lam / n, (1, blk_n))
    coef[1:2, :] = jnp.broadcast_to(mu, (1, blk_n))
    coef[2:3, :] = jnp.broadcast_to(jnp.full((1, 1), occ / n, jnp.float32), (1, blk_n))

    def first_x(mask, at):
        _, row, col = at
        blk = h_src(row, col)[...] if mask == 0 else buf[1, row, col]
        diag = eye * (row == col).astype(jnp.float32)
        val = coef[0:1, :] * (coef[1:2, :] * diag - blk) + coef[2:3, :] * diag
        buf[0, row, col] = val

        @pl.when(row != col)
        def _():
            buf[0, col, row] = val.T

        @pl.when(row == me)
        def _():
            hrow[col] = blk

        @pl.when(jnp.logical_and(col == me, row != me))
        def _():
            hrow[row] = blk.T

    def use(buf_id, row, col, turn):
        blk = buf[buf_id, row, col]
        x2row[col] += dot(buf[buf_id, me, row], blk, NN)

        @pl.when(row != col)
        def _():
            if turn:
                buf[buf_id, col, row] = blk.T
            x2row[row] += dot(buf[buf_id, me, col], blk, NT)

    def h_take(mask, at, t):
        if mask != 0:
            hx.arrive(mask, at, t)
        first_x(mask, at)

    def h_use(mask, at, t):
        use(0, *at[1:], False)

    def h_both(mask, at, t):
        h_take(mask, at, t)
        h_use(mask, at, t)

    early = [sources[k] * on + sources[XN + k] * (1 - on) for k in (0, PARTNER)]
    late = [sources[k] * (1 - on) + sources[XN + k] * on for k in (0, PARTNER)]
    @pl.loop(0, 4)
    def _(k):
        first_x(0, (me, 4 * y + k, me))

    hx.each([(mask, h_take) for mask in (0, PARTNER)])
    hx.each([(mask, h_take) for mask in (XN, YN, XN + 2, YN + 2)] + [(src, h_use) for src in early])
    hx.each([(src, h_use) for src in late + [sources[YN], sources[YN + 2]]] + [(DIAG, h_take)])
    hx.each([(DIAG, h_use), (DIAG + 2, h_both)])

    def product(old, col):
        tot = dot(x2row[0], buf[old, 0, col], NN)
        for k in range(1, PANELS):
            tot = tot + dot(x2row[k], buf[old, k, col], NN)
        return tot

    def traces(old, rnd):
        t1 = fold(buf[old, me, me] * eye)
        sums[...] = jnp.zeros_like(sums)

        @pl.loop(0, PANELS)
        def _(col):
            xv = buf[old, me, col]
            sums[0] += fold(xv * xv)
            sums[1] += fold(xv * x2row[col])

        sum_start(rnd, [t1, sums[0], sums[1]])

    def mix(rnd):
        t1, t2, t3 = sum_finish(rnd, 3)
        cval = (t2 - t3) / (t1 - t2)
        inv = 1.0 / (1.0 - cval)
        for k, val in enumerate(((1.0 - 2.0 * cval) * inv, (1.0 + cval) * inv, inv)):
            coef[k : k + 1, :] = jnp.broadcast_to(val, (1, blk_n))

    def updated(old, col):
        return coef[0:1, :] * buf[old, me, col] + coef[1:2, :] * x2row[col] - coef[2:3, :] * acc[...]

    before = hx
    for step in range(STEPS - 1):
        old, new = step % 2, (step + 1) % 2
        before.drain()
        traces(old, 1 + step)
        ex = Exchange(1 + step, new, x_place, lambda src: src.x_count)

        @pl.loop(0, SLOTS + 1)
        def _(t):
            at = ex.at(sources[0], t)
            col = at[2]
            acc[...] = product(old, col)

            @pl.when(t == 0)
            def _():
                mix(1 + step)

            buf[new, me, col] = updated(old, col)

            @pl.when(t < sources[0].x_count)
            def _():
                ex.own(at, t, lambda copy: copy.start())

        clear()

        def x_use(mask, at, t):
            use(new, *at[1:], True)

        def x_take(mask, at, t):
            ex.arrive(mask, at, t)
            _, row, col = at

            @pl.when(col == me)
            def _():
                buf[new, me, row] = buf[new, row, col].T

        def x_both(mask, at, t):
            ex.arrive(mask, at, t)
            x_use(mask, at, t)

        near = (PARTNER, XN, YN, XN + 2, YN + 2)
        ex.each([(0, x_use)])
        ex.each([(mask, x_take) for mask in near], 0, 2)
        ex.each([(mask, x_use) for mask in near], 0, 2)
        ex.each([(mask, x_both) for mask in near], 2, SLOTS)
        ex.each([(mask, x_both) for mask in (DIAG, DIAG + 2)])
        before = ex

    old, end = (STEPS - 1) % 2, STEPS % 2
    before.drain()
    traces(old, STEPS)
    sums[2] = jnp.zeros((8, 128), jnp.float32)

    def other(q, mask):
        return 4 * flip(half(q, 4), half(mask, 4)) + 2 * flip(part(half(q)), part(half(mask))) + flip(part(q), part(mask))

    def last_copy(q, mask, to):
        block = buf.at[end, q, other(q, mask)]
        return pltpu.make_async_remote_copy(
            src_ref=block,
            dst_ref=block,
            send_sem=last_send.at[mask],
            recv_sem=last_recv.at[mask],
            device_id=device(to),
            device_id_type=MESH,
        )

    def put(row, b, val):
        out_ref[span(row - 4 * y), span(b)] = val

    def last_mask(d):
        return on * pick(d, (5, 4, 7, 6, 3, 0, 1, 2)) + (1 - on) * pick(d, (0, 2, 4, 5, 6, 7, 1, 3))

    def last_send_to(d):
        return on * pick(d, (4, 1, 6, 1, 2)) + (1 - on)

    def last_sends(d):
        return d < 2 + 3 * on

    @pl.loop(0, PANELS)
    def _(d):
        @pl.when(d < 6 + 2 * on)
        def _():
            mask = last_mask(d)
            col = other(me, mask)
            acc[...] = product(old, col)

            @pl.when(d == 0)
            def _():
                mix(STEPS)

            val = updated(old, col)

            @pl.when(last_sends(d))
            def _():
                buf[end, me, col] = val

            weight = 1 + on * part(mask) * (1 - half(mask, 4))
            sums[2] += fold(val * hrow[col]) * weight.astype(jnp.float32)

            @pl.when(last_sends(d))
            def _():
                last_copy(me, mask, last_send_to(d)).start()

            @pl.when(half(col, 4) == y)
            def _():
                put(col, y, val.T)

            @pl.when(jnp.logical_and(on == 1, mask == 1))
            def _():
                put(me, 1 - y, val)

    sum_start(STEPS + 1, [sums[2]])

    @pl.when(on == 1)
    def _():
        for mask, src in ((3, 2), (0, 1), (2, 1)):
            q = sources[src].q
            last_copy(q, jnp.int32(mask), jnp.int32(src)).wait_recv()
            col = other(q, jnp.int32(mask))
            if mask == 3:
                put(q, 1 - y, buf[end, q, col])
            else:
                put(col, 1 - y, buf[end, q, col].T)

    @pl.when(on == 0)
    def _():
        for mask, src in ((5, 4), (4, 1), (7, 6), (6, 1)):
            q = sources[src].q
            last_copy(q, jnp.int32(mask), jnp.int32(src)).wait_recv()
            col = other(q, jnp.int32(mask))
            if src == YN:
                put(col, 1 - y, buf[end, q, col].T)
            else:
                put(q, 1 - y, buf[end, q, col])

    @pl.loop(0, SLOTS)
    def _(d):
        @pl.when(last_sends(d))
        def _():
            last_copy(me, last_mask(d), last_send_to(d)).wait_send()

    (energy,) = sum_finish(STEPS + 1, 1)
    e_ref[0] = 2.0 * jnp.sum(energy)


def solution(mesh):
    n_cols = mesh.shape["col"]

    def local_fn(ham_blk, bounds, n_occ):
        rows_n, cols_n = ham_blk.shape
        n = cols_n * n_cols
        blk_n = n // PANELS
        f32 = jnp.float32
        return pl.pallas_call(
            lambda *refs: kernel(n, *refs),
            out_shape=(jax.ShapeDtypeStruct((rows_n, cols_n), f32), jax.ShapeDtypeStruct((1,), f32)),
            in_specs=[
                pl.BlockSpec(memory_space=pltpu.SMEM),
                pl.BlockSpec(memory_space=pltpu.SMEM),
                pl.BlockSpec(memory_space=pltpu.VMEM),
            ],
            out_specs=(pl.BlockSpec(memory_space=pltpu.VMEM), pl.BlockSpec(memory_space=pltpu.SMEM)),
            scratch_shapes=[
                pltpu.VMEM((2, PANELS, PANELS, blk_n, blk_n), f32),
                pltpu.VMEM((PANELS, blk_n, blk_n), f32),
                pltpu.VMEM((PANELS, blk_n, blk_n), f32),
                pltpu.VMEM((blk_n, blk_n), f32),
                pltpu.VMEM((STEPS + 2, PANELS, 3, 8, 128), f32),
                pltpu.VMEM((8, blk_n), f32),
                pltpu.VMEM((3, 8, 128), f32),
                pltpu.SemaphoreType.DMA((3, PANELS, SLOTS, 3)),
                pltpu.SemaphoreType.DMA((3, PANELS, SLOTS)),
                pltpu.SemaphoreType.DMA((STEPS + 2, PANELS)),
                pltpu.SemaphoreType.DMA((STEPS + 2, PANELS)),
                pltpu.SemaphoreType.DMA((PANELS,)),
                pltpu.SemaphoreType.DMA((PANELS,)),
            ],
            compiler_params=pltpu.CompilerParams(collective_id=0, has_side_effects=True, vmem_limit_bytes=60 << 20),
            name="purify",
        )(bounds, n_occ, ham_blk)

    spec_mat = P(("spin", "row"), "col")
    return jax.shard_map(local_fn, mesh=mesh, in_specs=(spec_mat, P("spin"), P("spin")), out_specs=(spec_mat, P("spin")), check_vma=False)
```

```python
import jax
import jax.numpy as jnp
from jax import lax
from jax.experimental import pallas as pl
from jax.experimental.pallas import tpu as pltpu
from jax.sharding import PartitionSpec as P

STEPS = 3
PANELS = 8
SLOTS = 5
MESH = pl.DeviceIdType.MESH
NN = (((1,), (0,)), ((), ()))
NT = (((1,), (1,)), ((), ()))


def dot(lhs, rhs, dims):
    return lax.dot_general(lhs, rhs, dims, precision=lax.Precision.HIGHEST, preferred_element_type=jnp.float32)


def flag(cond):
    return lax.convert_element_type(cond, jnp.int32)


def pick(index, values):
    return sum(flag(index == k) * v for k, v in enumerate(values) if not (isinstance(v, int) and v == 0))


def half(val, by=2):
    return lax.div(val, jnp.int32(by))


def part(val, by=2):
    return lax.rem(val, jnp.int32(by))


def flip(bit, by):
    return bit + by - 2 * bit * by


def panel_bits(q):
    return q // 4, q % 2, (q // 2) % 2


def packed(digits, base):
    return sum(d * base**k for k, d in enumerate(digits))


def h_blocks(q):
    x, y, c = panel_bits(q)
    if x == y:
        local = {
            (0, 0): ((1, 1), (1, 0), (3, 0), (0, 0), (2, 0)),
            (0, 1): ((3, 1), (3, 0), (1, 0), (1, 1), (2, 0)),
            (1, 0): ((0, 0), (1, 0), (2, 0), (3, 0), (1, 1)),
            (1, 1): ((2, 0), (3, 0), (1, 0), (3, 1), (1, 1)),
        }[x, c]
    else:
        local = tuple((2 * k + (b + y) % 2, b) for b in range(2) for k in range(2))
    return tuple((4 * y + a, 4 * x + 2 * c + b) for a, b in local)


def x_blocks(q):
    x, y, c = panel_bits(q)
    return tuple(q ^ m for m in (4 + 2 * x, 1 + 2 * y, 5 + 2 * y, 0, 2, 7 - 2 * y))


def kernel(n, bounds, n_occ, h_ref, out_ref, e_ref, buf, hrow, x2row, acc, parts, coef, sums, send_sem, recv_sem, part_send, part_recv, last_send, last_recv):
    blk_n = n // PANELS
    y = lax.axis_index("row")
    j = lax.axis_index("col")
    x, c = half(j), part(j)
    me = 4 * x + 2 * c + y
    on = 1 - flip(x, y)

    class Source:
        def __init__(self, q, h_pack, h_count, x_pack, x_count):
            self.fields = q, h_pack, h_count, x_pack, x_count
            self.q, self.h_pack, self.h_count, self.x_pack, self.x_count = self.fields

        def __add__(self, other):
            return Source(*(a + b for a, b in zip(self.fields, other.fields)))

        def __mul__(self, by):
            return Source(*(a * by for a in self.fields))

    def device(mask):
        dx, dy, dc = flip(x, half(mask, 4)), flip(y, part(mask)), flip(c, part(half(mask)))
        return (0, dy, 2 * dx + dc)

    def source(mask):
        q = panel(mask)
        return Source(
            q,
            pick(q, [packed([8 * row + col for row, col in h_blocks(k)], 64) for k in range(PANELS)]),
            pick(q, [len(h_blocks(k)) for k in range(PANELS)]),
            pick(q, [packed(x_blocks(k), 8) for k in range(PANELS)]),
            pick(q, [5 - (k // 2) % 2 for k in range(PANELS)]),
        )

    def panel(mask):
        return 4 * flip(x, mask // 4) + 2 * flip(c, (mask // 2) % 2) + flip(y, mask % 2)

    def h_place(src, t):
        code = part(lax.div(src.h_pack, pick(t, [64**k for k in range(SLOTS)])), 64)
        return half(code, 8), part(code, 8)

    def x_place(src, t):
        return src.q, part(lax.div(src.x_pack, pick(t, [8**k for k in range(SLOTS + 1)])), 8)

    devices = [device(jnp.int32(mask)) for mask in range(8)]
    sources = [source(mask) for mask in range(8)]

    PARTNER, XN, YN, DIAG = 2, 4, 1, 5

    barrier = pltpu.get_barrier_semaphore()
    for mask in range(1, 8):
        pl.semaphore_signal(barrier, inc=1, device_id=devices[mask], device_id_type=MESH)
    pl.semaphore_wait(barrier, 7)

    class Exchange:
        def __init__(self, rnd, buf_id, place, count, own_src=None):
            self.rnd, self.buf_id, self.place, self.count = rnd, buf_id, place, count
            self.own_src = own_src or (lambda row, col: buf.at[buf_id, row, col])

        def copy(self, at, t, way, src=None):
            q, row, col = at
            block = buf.at[self.buf_id, row, col]
            return pltpu.make_async_remote_copy(
                src_ref=block if src is None else src,
                dst_ref=block,
                send_sem=send_sem.at[self.rnd, q, t, way],
                recv_sem=recv_sem.at[self.rnd, q, t],
                device_id=devices[(PARTNER, XN, YN)[way]],
                device_id_type=MESH,
            )

        def own(self, at, t, act):
            for way in range(3):
                act(self.copy(at, t, way, self.own_src(*at[1:])))

        def forward(self, mask, at, t, act):
            if mask in (XN, YN, DIAG):
                act(self.copy(at, t, 0))
            if mask == XN:

                @pl.when(part(t) + flag(t == 4) * y == 0)
                def _():
                    act(self.copy(at, t, 2))

            if mask == YN:

                @pl.when(part(t) + flag(t == 4) * (1 - y) == 1)
                def _():
                    act(self.copy(at, t, 1))

        def forward_any(self, k, masks, at, t, act):
            for mask in (XN, YN, DIAG):
                if mask in masks:

                    @pl.when(k == masks.index(mask))
                    def _():
                        self.forward(mask, at, t, act)

        def arrive(self, k, masks, at, t):
            self.copy(at, t, 0).wait_recv()
            self.forward_any(k, masks, at, t, lambda copy: copy.start())

        def at(self, src, t):
            return (src.q, *self.place(src, t))

        def each(self, masks, body, first=0, last=SLOTS):
            srcs = [mask if isinstance(mask, Source) else sources[mask] for mask in masks]
            many = len(srcs)

            @pl.loop(0, (last - first) * many)
            def _(i):
                t, k = first + half(i, many), part(i, many)
                src = srcs[0] if many == 1 else Source(*(pick(k, vals) for vals in zip(*(src.fields for src in srcs))))

                @pl.when(t < self.count(src))
                def _():
                    body(k, self.at(src, t), t)

        def drain(self):
            self.each((0,), lambda k, at, t: self.own(at, t, lambda copy: copy.wait_send()))
            far = (XN, YN, DIAG)
            self.each(far, lambda k, at, t: self.forward_any(k, far, at, t, lambda copy: copy.wait_send()))

    def part_copy(rnd, src, mask):
        return pltpu.make_async_remote_copy(
            src_ref=parts.at[rnd, src],
            dst_ref=parts.at[rnd, src],
            send_sem=part_send.at[rnd, mask],
            recv_sem=part_recv.at[rnd, src],
            device_id=devices[mask],
            device_id_type=MESH,
        )

    def sum_start(rnd, vals):
        for k, val in enumerate(vals):
            parts[rnd, me, k] = val
        for mask in range(1, 8):
            part_copy(rnd, me, mask).start()

    def sum_finish(rnd, count):
        for mask in range(1, 8):
            part_copy(rnd, sources[mask].q, mask).wait_recv()
        for mask in range(1, 8):
            part_copy(rnd, me, mask).wait_send()
        out = []
        for k in range(count):
            tot = parts[rnd, 0, k]
            for q in range(1, PANELS):
                tot = tot + parts[rnd, q, k]
            out.append(jnp.sum(jnp.sum(tot, axis=1, keepdims=True), axis=0, keepdims=True))
        return out

    def fold(val):
        rows, cols = val.shape
        val = jnp.sum(val.reshape(rows // 8, 8, cols), axis=0)
        tot = val[:, :128]
        for k in range(1, cols // 128):
            tot = tot + val[:, k * 128 : (k + 1) * 128]
        return tot

    def span(k):
        return pl.ds(pl.multiple_of(k * blk_n, blk_n), blk_n)

    def clear():
        @pl.loop(0, PANELS)
        def _(col):
            x2row[col] = jnp.zeros((blk_n, blk_n), jnp.float32)

    def h_src(row, col):
        return h_ref.at[span(row - 4 * y), span(col - 2 * j)]

    hx = Exchange(0, 1, h_place, lambda src: src.h_count, h_src)
    hx.each((0,), lambda k, at, t: hx.own(at, t, lambda copy: copy.start()))

    rows_n, cols_n = h_ref.shape
    mu_part = jnp.zeros((8, 128), jnp.float32)
    for k in range(rows_n // blk_n):
        tile = h_ref[k * blk_n : (k + 1) * blk_n, :]
        row_ids = y * rows_n + k * blk_n + lax.broadcasted_iota(jnp.int32, tile.shape, 0)
        col_ids = j * cols_n + lax.broadcasted_iota(jnp.int32, tile.shape, 1)
        mu_part = mu_part + fold(jnp.where(row_ids == col_ids, tile, 0.0))
    sum_start(0, [mu_part])
    clear()

    eye = (lax.broadcasted_iota(jnp.int32, (blk_n, blk_n), 0) == lax.broadcasted_iota(jnp.int32, (blk_n, blk_n), 1)).astype(jnp.float32)
    (trace_h,) = sum_finish(0, 1)
    occ = n_occ[0].astype(jnp.float32)
    mu = trace_h / n
    lam = jnp.minimum(occ / (bounds[1] - mu), (n - occ) / (mu - bounds[0]))
    coef[0:1, :] = jnp.broadcast_to(lam / n, (1, blk_n))
    coef[1:2, :] = jnp.broadcast_to(mu, (1, blk_n))
    coef[2:3, :] = jnp.broadcast_to(jnp.full((1, 1), occ / n, jnp.float32), (1, blk_n))

    def first_x(own, at):
        _, row, col = at
        blk = h_src(row, col)[...] if own else buf[1, row, col]
        diag = eye * (row == col).astype(jnp.float32)
        val = coef[0:1, :] * (coef[1:2, :] * diag - blk) + coef[2:3, :] * diag
        buf[0, row, col] = val

        @pl.when(row != col)
        def _():
            buf[0, col, row] = val.T

        @pl.when(row == me)
        def _():
            hrow[col] = blk

        @pl.when(jnp.logical_and(col == me, row != me))
        def _():
            hrow[row] = blk.T

    def use(buf_id, row, col, turn):
        blk = buf[buf_id, row, col]
        x2row[col] += dot(buf[buf_id, me, row], blk, NN)

        @pl.when(row != col)
        def _():
            if turn:
                buf[buf_id, col, row] = blk.T
            x2row[row] += dot(buf[buf_id, me, col], blk, NT)

    def h_take(masks):
        def body(k, at, t):
            hx.arrive(k, masks, at, t)
            first_x(False, at)

        return body

    def h_use(k, at, t):
        use(0, *at[1:], False)

    @pl.loop(0, 4)
    def _(k):
        first_x(True, (me, 4 * y + k, me))

    hx.each((0,), lambda k, at, t: first_x(True, at))
    hx.each((PARTNER,), h_take((PARTNER,)))

    early = [sources[k] * on + sources[XN + k] * (1 - on) for k in (0, PARTNER)]
    late = [sources[k] * (1 - on) + sources[XN + k] * on for k in (0, PARTNER)]
    near = (XN, YN, XN + 2, YN + 2)

    @pl.loop(0, SLOTS)
    def _(t):
        hx.each(near, h_take(near), t, t + 1)
        hx.each(early, h_use, t, t + 1)

    @pl.loop(0, SLOTS)
    def _(t):
        hx.each(late + [sources[YN], sources[YN + 2]], h_use, t, t + 1)
        hx.each((DIAG,), h_take((DIAG,)), t, t + 1)

    @pl.loop(0, SLOTS)
    def _(t):
        hx.each((DIAG + 2,), h_take((DIAG + 2,)), t, t + 1)
        hx.each((DIAG, DIAG + 2), h_use, t, t + 1)

    def product(old, col):
        tot = dot(x2row[0], buf[old, 0, col], NN)
        for k in range(1, PANELS):
            tot = tot + dot(x2row[k], buf[old, k, col], NN)
        return tot

    def traces(old, rnd):
        t1 = fold(buf[old, me, me] * eye)
        sums[...] = jnp.zeros_like(sums)

        @pl.loop(0, PANELS)
        def _(col):
            xv = buf[old, me, col]
            sums[0] += fold(xv * xv)
            sums[1] += fold(xv * x2row[col])

        sum_start(rnd, [t1, sums[0], sums[1]])

    def mix(rnd):
        t1, t2, t3 = sum_finish(rnd, 3)
        cval = (t2 - t3) / (t1 - t2)
        inv = 1.0 / (1.0 - cval)
        for k, val in enumerate(((1.0 - 2.0 * cval) * inv, (1.0 + cval) * inv, inv)):
            coef[k : k + 1, :] = jnp.broadcast_to(val, (1, blk_n))

    def updated(old, col):
        return coef[0:1, :] * buf[old, me, col] + coef[1:2, :] * x2row[col] - coef[2:3, :] * acc[...]

    before = hx
    for step in range(STEPS - 1):
        old, new = step % 2, (step + 1) % 2
        before.drain()
        traces(old, 1 + step)
        ex = Exchange(1 + step, new, x_place, lambda src: src.x_count)

        @pl.loop(0, SLOTS + 1)
        def _(t):
            at = ex.at(sources[0], t)
            col = at[2]
            acc[...] = product(old, col)

            @pl.when(t == 0)
            def _():
                mix(1 + step)

            buf[new, me, col] = updated(old, col)

            @pl.when(t < sources[0].x_count)
            def _():
                ex.own(at, t, lambda copy: copy.start())

        clear()

        def x_use(k, at, t):
            use(new, *at[1:], True)

        def x_take(masks):
            def body(k, at, t):
                ex.arrive(k, masks, at, t)
                _, row, col = at

                @pl.when(col == me)
                def _():
                    buf[new, me, row] = buf[new, row, col].T

            return body

        def x_both(masks):
            def body(k, at, t):
                ex.arrive(k, masks, at, t)
                use(new, *at[1:], True)

            return body

        near = (PARTNER, XN, YN, XN + 2, YN + 2)
        far = (DIAG, DIAG + 2)
        ex.each((0,), x_use)
        ex.each(near, x_take(near), 0, 2)
        ex.each(near, x_use, 0, 2)
        ex.each(near, x_both(near), 2, SLOTS)
        ex.each(far, x_both(far))
        before = ex

    old, end = (STEPS - 1) % 2, STEPS % 2
    before.drain()
    traces(old, STEPS)
    sums[2] = jnp.zeros((8, 128), jnp.float32)

    def other(q, mask):
        return 4 * flip(half(q, 4), half(mask, 4)) + 2 * flip(part(half(q)), part(half(mask))) + flip(part(q), part(mask))

    def last_copy(q, mask, to):
        block = buf.at[end, q, other(q, mask)]
        return pltpu.make_async_remote_copy(
            src_ref=block,
            dst_ref=block,
            send_sem=last_send.at[mask],
            recv_sem=last_recv.at[mask],
            device_id=device(to),
            device_id_type=MESH,
        )

    def put(row, b, val):
        out_ref[span(row - 4 * y), span(b)] = val

    def last_mask(d):
        return on * pick(d, (5, 4, 7, 6, 3, 0, 1, 2)) + (1 - on) * pick(d, (0, 2, 4, 5, 6, 7, 1, 3))

    def last_send_to(d):
        return on * pick(d, (4, 1, 6, 1, 2)) + (1 - on)

    def last_sends(d):
        return d < 2 + 3 * on

    @pl.loop(0, PANELS)
    def _(d):
        @pl.when(d < 6 + 2 * on)
        def _():
            mask = last_mask(d)
            col = other(me, mask)
            acc[...] = product(old, col)

            @pl.when(d == 0)
            def _():
                mix(STEPS)

            val = updated(old, col)

            @pl.when(last_sends(d))
            def _():
                buf[end, me, col] = val

            weight = 1 + on * part(mask) * (1 - half(mask, 4))
            sums[2] += fold(val * hrow[col]) * weight.astype(jnp.float32)

            @pl.when(last_sends(d))
            def _():
                last_copy(me, mask, last_send_to(d)).start()

            @pl.when(half(col, 4) == y)
            def _():
                put(col, y, val.T)

            @pl.when(jnp.logical_and(on == 1, mask == 1))
            def _():
                put(me, 1 - y, val)

    sum_start(STEPS + 1, [sums[2]])

    @pl.when(on == 1)
    def _():
        for mask, src in ((3, 2), (0, 1), (2, 1)):
            q = sources[src].q
            last_copy(q, jnp.int32(mask), jnp.int32(src)).wait_recv()
            col = other(q, jnp.int32(mask))
            if mask == 3:
                put(q, 1 - y, buf[end, q, col])
            else:
                put(col, 1 - y, buf[end, q, col].T)

    @pl.when(on == 0)
    def _():
        for mask, src in ((5, 4), (4, 1), (7, 6), (6, 1)):
            q = sources[src].q
            last_copy(q, jnp.int32(mask), jnp.int32(src)).wait_recv()
            col = other(q, jnp.int32(mask))
            if src == YN:
                put(col, 1 - y, buf[end, q, col].T)
            else:
                put(q, 1 - y, buf[end, q, col])

    @pl.loop(0, SLOTS)
    def _(d):
        @pl.when(last_sends(d))
        def _():
            last_copy(me, last_mask(d), last_send_to(d)).wait_send()

    (energy,) = sum_finish(STEPS + 1, 1)
    e_ref[0] = 2.0 * jnp.sum(energy)


def solution(mesh):
    n_cols = mesh.shape["col"]

    def local_fn(ham_blk, bounds, n_occ):
        rows_n, cols_n = ham_blk.shape
        n = cols_n * n_cols
        blk_n = n // PANELS
        f32 = jnp.float32
        return pl.pallas_call(
            lambda *refs: kernel(n, *refs),
            out_shape=(jax.ShapeDtypeStruct((rows_n, cols_n), f32), jax.ShapeDtypeStruct((1,), f32)),
            in_specs=[
                pl.BlockSpec(memory_space=pltpu.SMEM),
                pl.BlockSpec(memory_space=pltpu.SMEM),
                pl.BlockSpec(memory_space=pltpu.VMEM),
            ],
            out_specs=(pl.BlockSpec(memory_space=pltpu.VMEM), pl.BlockSpec(memory_space=pltpu.SMEM)),
            scratch_shapes=[
                pltpu.VMEM((2, PANELS, PANELS, blk_n, blk_n), f32),
                pltpu.VMEM((PANELS, blk_n, blk_n), f32),
                pltpu.VMEM((PANELS, blk_n, blk_n), f32),
                pltpu.VMEM((blk_n, blk_n), f32),
                pltpu.VMEM((STEPS + 2, PANELS, 3, 8, 128), f32),
                pltpu.VMEM((8, blk_n), f32),
                pltpu.VMEM((3, 8, 128), f32),
                pltpu.SemaphoreType.DMA((3, PANELS, SLOTS, 3)),
                pltpu.SemaphoreType.DMA((3, PANELS, SLOTS)),
                pltpu.SemaphoreType.DMA((STEPS + 2, PANELS)),
                pltpu.SemaphoreType.DMA((STEPS + 2, PANELS)),
                pltpu.SemaphoreType.DMA((PANELS,)),
                pltpu.SemaphoreType.DMA((PANELS,)),
            ],
            compiler_params=pltpu.CompilerParams(collective_id=0, has_side_effects=True, vmem_limit_bytes=60 << 20),
            name="purify",
        )(bounds, n_occ, ham_blk)

    spec_mat = P(("spin", "row"), "col")
    return jax.shard_map(local_fn, mesh=mesh, in_specs=(spec_mat, P("spin"), P("spin")), out_specs=(spec_mat, P("spin")), check_vma=False)
```

```python
import jax
import jax.numpy as jnp
from jax import lax
from jax.experimental import pallas as pl
from jax.experimental.pallas import tpu as pltpu
from jax.sharding import PartitionSpec as P

STEPS = 3
PANELS = 8
SLOTS = 5
MESH = pl.DeviceIdType.MESH
NN = (((1,), (0,)), ((), ()))
NT = (((1,), (1,)), ((), ()))


def dot(lhs, rhs, dims):
    return lax.dot_general(lhs, rhs, dims, precision=lax.Precision.HIGHEST, preferred_element_type=jnp.float32)


def flag(cond):
    return lax.convert_element_type(cond, jnp.int32)


def pick(index, values):
    return sum(flag(index == k) * v for k, v in enumerate(values) if not (isinstance(v, int) and v == 0))


def half(val, by=2):
    return lax.div(val, jnp.int32(by))


def part(val, by=2):
    return lax.rem(val, jnp.int32(by))


def flip(bit, by):
    return bit + by - 2 * bit * by


def panel_bits(q):
    return q // 4, q % 2, (q // 2) % 2


def packed(digits, base):
    return sum(d * base**k for k, d in enumerate(digits))


def h_blocks(q):
    x, y, c = panel_bits(q)
    if x == y:
        local = {
            (0, 0): ((1, 1), (1, 0), (3, 0), (0, 0), (2, 0)),
            (0, 1): ((3, 1), (3, 0), (1, 0), (1, 1), (2, 0)),
            (1, 0): ((0, 0), (1, 0), (2, 0), (3, 0), (1, 1)),
            (1, 1): ((2, 0), (3, 0), (1, 0), (3, 1), (1, 1)),
        }[x, c]
    else:
        local = tuple((2 * k + (b + y) % 2, b) for b in range(2) for k in range(2))
    return tuple((4 * y + a, 4 * x + 2 * c + b) for a, b in local)


def x_blocks(q):
    x, y, c = panel_bits(q)
    return tuple(q ^ m for m in (4 + 2 * x, 1 + 2 * y, 5 + 2 * y, 0, 2, 7 - 2 * y))


def kernel(n, bounds, n_occ, h_ref, out_ref, e_ref, buf, hrow, x2row, acc, parts, coef, sums, send_sem, recv_sem, part_send, part_recv, last_send, last_recv):
    blk_n = n // PANELS
    y = lax.axis_index("row")
    j = lax.axis_index("col")
    x, c = half(j), part(j)
    me = 4 * x + 2 * c + y
    on = 1 - flip(x, y)

    class Source:
        def __init__(self, q, h_pack, h_count, x_pack, x_count):
            self.fields = q, h_pack, h_count, x_pack, x_count
            self.q, self.h_pack, self.h_count, self.x_pack, self.x_count = self.fields

        def __add__(self, other):
            return Source(*(a + b for a, b in zip(self.fields, other.fields)))

        def __mul__(self, by):
            return Source(*(a * by for a in self.fields))

    def device(mask):
        dx, dy, dc = flip(x, half(mask, 4)), flip(y, part(mask)), flip(c, part(half(mask)))
        return (0, dy, 2 * dx + dc)

    def source(mask):
        q = panel(mask)
        return Source(
            q,
            pick(q, [packed([8 * row + col for row, col in h_blocks(k)], 64) for k in range(PANELS)]),
            pick(q, [len(h_blocks(k)) for k in range(PANELS)]),
            pick(q, [packed(x_blocks(k), 8) for k in range(PANELS)]),
            pick(q, [5 - (k // 2) % 2 for k in range(PANELS)]),
        )

    def panel(mask):
        return 4 * flip(x, mask // 4) + 2 * flip(c, (mask // 2) % 2) + flip(y, mask % 2)

    def h_place(src, t):
        code = part(lax.div(src.h_pack, pick(t, [64**k for k in range(SLOTS)])), 64)
        return half(code, 8), part(code, 8)

    def x_place(src, t):
        return src.q, part(lax.div(src.x_pack, pick(t, [8**k for k in range(SLOTS + 1)])), 8)

    devices = [device(jnp.int32(mask)) for mask in range(8)]
    sources = [source(mask) for mask in range(8)]

    PARTNER, XN, YN, DIAG = 2, 4, 1, 5

    barrier = pltpu.get_barrier_semaphore()
    for mask in range(1, 8):
        pl.semaphore_signal(barrier, inc=1, device_id=devices[mask], device_id_type=MESH)
    pl.semaphore_wait(barrier, 7)

    class Exchange:
        def __init__(self, rnd, buf_id, place, count, own_src=None):
            self.rnd, self.buf_id, self.place, self.count = rnd, buf_id, place, count
            self.own_src = own_src or (lambda row, col: buf.at[buf_id, row, col])

        def copy(self, at, t, way, src=None):
            q, row, col, _ = at
            block = buf.at[self.buf_id, row, col]
            return pltpu.make_async_remote_copy(
                src_ref=block if src is None else src,
                dst_ref=block,
                send_sem=send_sem.at[self.rnd % 2, q, t, way],
                recv_sem=recv_sem.at[self.rnd % 2, q, t],
                device_id=devices[(PARTNER, XN, YN)[way]],
                device_id_type=MESH,
            )

        def own(self, at, t, act):
            for way in range(3):
                act(self.copy(at, t, way, self.own_src(*at[1:3])))

        def forward(self, mask, at, t, act):
            if mask in (XN, YN, DIAG):
                act(self.copy(at, t, 0))
            if mask == XN:

                @pl.when(part(t) + flag(t == 4) * y == 0)
                def _():
                    act(self.copy(at, t, 2))

            if mask == YN:

                @pl.when(part(t) + flag(t == 4) * (1 - y) == 1)
                def _():
                    act(self.copy(at, t, 1))

        def forward_any(self, k, masks, at, t, act):
            for mask in (XN, YN, DIAG):
                if mask in masks:

                    @pl.when(k == masks.index(mask))
                    def _():
                        self.forward(mask, at, t, act)

        def arrive(self, k, masks, at, t):
            self.copy(at, t, 0).wait_recv()
            self.forward_any(k, masks, at, t, lambda copy: copy.start())

        def at(self, src, t):
            return (src.q, *self.place(src, t), src)

        def each(self, masks, body, first=0, last=SLOTS):
            srcs = [mask if isinstance(mask, Source) else sources[mask] for mask in masks]
            many = len(srcs)

            @pl.loop(0, (last - first) * many)
            def _(i):
                t, k = first + half(i, many), part(i, many)
                src = srcs[0] if many == 1 else Source(*(pick(k, vals) for vals in zip(*(src.fields for src in srcs))))

                @pl.when(t < self.count(src))
                def _():
                    body(k, self.at(src, t), t)

        def drain(self):
            self.each((0,), lambda k, at, t: self.own(at, t, lambda copy: copy.wait_send()))
            far = (XN, YN, DIAG)
            self.each(far, lambda k, at, t: self.forward_any(k, far, at, t, lambda copy: copy.wait_send()))

    def part_copy(rnd, src, mask):
        return pltpu.make_async_remote_copy(
            src_ref=parts.at[rnd, src],
            dst_ref=parts.at[rnd, src],
            send_sem=part_send.at[rnd, mask],
            recv_sem=part_recv.at[rnd, src],
            device_id=devices[mask],
            device_id_type=MESH,
        )

    def sum_start(rnd, vals):
        for k, val in enumerate(vals):
            parts[rnd, me, k] = val
        for mask in range(1, 8):
            part_copy(rnd, me, mask).start()

    def sum_finish(rnd, count):
        for mask in range(1, 8):
            part_copy(rnd, sources[mask].q, mask).wait_recv()
        for mask in range(1, 8):
            part_copy(rnd, me, mask).wait_send()
        out = []
        for k in range(count):
            tot = parts[rnd, 0, k]
            for q in range(1, PANELS):
                tot = tot + parts[rnd, q, k]
            out.append(jnp.sum(jnp.sum(tot, axis=1, keepdims=True), axis=0, keepdims=True))
        return out

    def fold(val):
        rows, cols = val.shape
        val = jnp.sum(val.reshape(rows // 8, 8, cols), axis=0)
        tot = val[:, :128]
        for k in range(1, cols // 128):
            tot = tot + val[:, k * 128 : (k + 1) * 128]
        return tot

    def span(k):
        return pl.ds(pl.multiple_of(k * blk_n, blk_n), blk_n)

    def clear():
        @pl.loop(0, PANELS)
        def _(col):
            x2row[col] = jnp.zeros((blk_n, blk_n), jnp.float32)

    def h_src(row, col):
        return h_ref.at[span(row - 4 * y), span(col - 2 * j)]

    hx = Exchange(0, 1, h_place, lambda src: src.h_count, h_src)
    hx.each((0,), lambda k, at, t: hx.own(at, t, lambda copy: copy.start()))

    rows_n, cols_n = h_ref.shape
    mu_part = jnp.zeros((8, 128), jnp.float32)
    for k in range(rows_n // blk_n):
        tile = h_ref[k * blk_n : (k + 1) * blk_n, :]
        row_ids = y * rows_n + k * blk_n + lax.broadcasted_iota(jnp.int32, tile.shape, 0)
        col_ids = j * cols_n + lax.broadcasted_iota(jnp.int32, tile.shape, 1)
        mu_part = mu_part + fold(jnp.where(row_ids == col_ids, tile, 0.0))
    sum_start(0, [mu_part])
    clear()

    eye = (lax.broadcasted_iota(jnp.int32, (blk_n, blk_n), 0) == lax.broadcasted_iota(jnp.int32, (blk_n, blk_n), 1)).astype(jnp.float32)
    (trace_h,) = sum_finish(0, 1)
    occ = n_occ[0].astype(jnp.float32)
    mu = trace_h / n
    lam = jnp.minimum(occ / (bounds[1] - mu), (n - occ) / (mu - bounds[0]))
    coef[0:1, :] = jnp.broadcast_to(lam / n, (1, blk_n))
    coef[1:2, :] = jnp.broadcast_to(mu, (1, blk_n))
    coef[2:3, :] = jnp.broadcast_to(jnp.full((1, 1), occ / n, jnp.float32), (1, blk_n))

    def first_x(own, at):
        _, row, col = at[:3]
        blk = h_src(row, col)[...] if own else buf[1, row, col]
        diag = eye * (row == col).astype(jnp.float32)
        val = coef[0:1, :] * (coef[1:2, :] * diag - blk) + coef[2:3, :] * diag
        buf[0, row, col] = val

        @pl.when(row != col)
        def _():
            buf[0, col, row] = val.T

        @pl.when(row == me)
        def _():
            hrow[col] = blk

        @pl.when(jnp.logical_and(col == me, row != me))
        def _():
            hrow[row] = blk.T

    def use(b, row, col):
        blk = buf[b, row, col]
        x2row[col] += dot(buf[b, me, row], blk, NN)
        x2row[row] += dot(buf[b, me, col], blk, NT)
        buf[b, col, row] = blk.T

    def use_pair(b, row, col):
        blk = [buf[b, row, k] for k in col]
        left = buf[b, me, row]
        right = [buf[b, me, k] for k in col]
        for k in range(2):
            x2row[col[k]] += dot(left, blk[k], NN)
        x2row[row] += dot(right[0], blk[0], NT) + dot(right[1], blk[1], NT)
        for k in range(2):
            buf[b, col[k], row] = blk[k].T

    def use_diag(b, row, col):
        blk, mid = buf[b, row, col], buf[b, row, row]
        left = buf[b, me, row]
        right = buf[b, me, col]
        x2row[col] += dot(left, blk, NN)
        x2row[row] += dot(right, blk, NT) + dot(left, mid, NN)
        buf[b, col, row] = blk.T

    def h_take(masks):
        def body(k, at, t):
            hx.arrive(k, masks, at, t)
            first_x(False, at)

        return body

    def h_unit(col, kind):
        cross = half(kind)
        first = 4 * flip(half(col, 4), cross) + (1 - cross) * 2 * kind + cross * flip(part(col), part(kind))
        second = first + 1 + cross
        x2row[col] += dot(buf[0, me, first], buf[0, first, col], NN) + dot(buf[0, me, second], buf[0, second, col], NN)

    @pl.loop(0, 4)
    def _(k):
        first_x(True, (me, 4 * y + k, me))

    hx.each((0,), lambda k, at, t: first_x(True, at))
    hx.each((PARTNER,), h_take((PARTNER,)))

    near = (XN, YN, XN + 2, YN + 2)
    far = (DIAG, DIAG + 2)
    off = 1 - on
    hx.each(near, h_take(near), 0, 1)

    @pl.loop(0, 4 + 4 * on)
    def _(i):
        h_unit(on * (4 * y + half(i)) + off * (4 - 4 * y + i), on * part(i) + off * (2 + y))

    hx.each(near, h_take(near), 1, SLOTS)

    @pl.loop(0, 16)
    def _(i):
        h_unit(on * (4 * flip(y, half(i, 8)) + half(part(i, 8))) + off * half(i), on * 2 + part(i))

    @pl.loop(0, 4 * off)
    def _(i):
        h_unit(4 * y + i, 2 + y)

    hx.each(far, h_take(far))

    @pl.loop(0, 8)
    def _(i):
        h_unit(on * (4 - 4 * y + half(i)) + off * i, on * part(i) + off * (3 - y))

    def product(old, col):
        tot = dot(x2row[0], buf[old, 0, col], NN)
        for k in range(1, PANELS):
            tot = tot + dot(x2row[k], buf[old, k, col], NN)
        return tot

    def traces(old, rnd):
        t1 = fold(buf[old, me, me] * eye)
        sums[...] = jnp.zeros_like(sums)

        @pl.loop(0, PANELS)
        def _(col):
            xv = buf[old, me, col]
            sums[0] += fold(xv * xv)
            sums[1] += fold(xv * x2row[col])

        sum_start(rnd, [t1, sums[0], sums[1]])

    def mix(rnd):
        t1, t2, t3 = sum_finish(rnd, 3)
        cval = (t2 - t3) / (t1 - t2)
        inv = 1.0 / (1.0 - cval)
        for k, val in enumerate(((1.0 - 2.0 * cval) * inv, (1.0 + cval) * inv, inv)):
            coef[k : k + 1, :] = jnp.broadcast_to(val, (1, blk_n))

    def updated(old, col):
        return coef[0:1, :] * buf[old, me, col] + coef[1:2, :] * x2row[col] - coef[2:3, :] * acc[...]

    before = hx
    for step in range(STEPS - 1):
        old, new = step % 2, (step + 1) % 2
        before.drain()
        traces(old, 1 + step)
        ex = Exchange(1 + step, new, x_place, lambda src: src.x_count)

        @pl.loop(0, SLOTS + 1)
        def _(t):
            at = ex.at(sources[0], t)
            col = at[2]
            acc[...] = product(old, col)

            @pl.when(t == 0)
            def _():
                mix(1 + step)

            buf[new, me, col] = updated(old, col)

            @pl.when(t < sources[0].x_count)
            def _():
                ex.own(at, t, lambda copy: copy.start())

        clear()

        def x_take(masks):
            def body(k, at, t):
                ex.arrive(k, masks, at, t)
                _, row, col = at[:3]

                @pl.when(col == me)
                def _():
                    buf[new, me, row] = buf[new, row, col].T

            return body

        def x_first(k, at, t):
            src = at[3]
            use_pair(new, at[1], (at[2], x_place(src, 1)[1]))

        def x_second(k, at, t):
            use_diag(new, at[1], at[2])

        def x_last(k, at, t):
            use(new, at[1], at[2])

        near = (PARTNER, XN, YN, XN + 2, YN + 2)
        far = (DIAG, DIAG + 2)
        ex.each((0,), x_first, 0, 1)
        ex.each(near, x_take(near), 0, 2)
        ex.each(near, x_first, 0, 1)
        ex.each(near, x_take(near), 2, 4)
        ex.each((0, *near), x_second, 2, 3)
        ex.each(near, x_take(near), 4, 5)
        ex.each((0, *near), x_last, 4, 5)
        ex.each(far, x_take(far), 0, 2)
        ex.each(far, x_first, 0, 1)
        ex.each(far, x_take(far), 2, 4)
        ex.each(far, x_second, 2, 3)
        ex.each(far, x_take(far), 4, 5)
        ex.each(far, x_last, 4, 5)
        before = ex

    old, end = (STEPS - 1) % 2, STEPS % 2
    before.drain()
    traces(old, STEPS)
    sums[2] = jnp.zeros((8, 128), jnp.float32)

    def other(q, mask):
        return 4 * flip(half(q, 4), half(mask, 4)) + 2 * flip(part(half(q)), part(half(mask))) + flip(part(q), part(mask))

    def last_copy(q, mask, to):
        block = buf.at[end, q, other(q, mask)]
        return pltpu.make_async_remote_copy(
            src_ref=block,
            dst_ref=block,
            send_sem=last_send.at[mask],
            recv_sem=last_recv.at[mask],
            device_id=device(to),
            device_id_type=MESH,
        )

    def put(row, b, val):
        out_ref[span(row - 4 * y), span(b)] = val

    def last_mask(d):
        return on * pick(d, (5, 4, 7, 6, 3, 0, 1, 2)) + (1 - on) * pick(d, (0, 2, 4, 5, 6, 7, 1, 3))

    def last_send_to(d):
        return on * pick(d, (4, 1, 6, 1, 2)) + (1 - on)

    def last_sends(d):
        return d < 2 + 3 * on

    @pl.loop(0, PANELS)
    def _(d):
        @pl.when(d < 6 + 2 * on)
        def _():
            mask = last_mask(d)
            col = other(me, mask)
            acc[...] = product(old, col)

            @pl.when(d == 0)
            def _():
                mix(STEPS)

            val = updated(old, col)

            @pl.when(last_sends(d))
            def _():
                buf[end, me, col] = val

            weight = 1 + on * part(mask) * (1 - half(mask, 4))
            sums[2] += fold(val * hrow[col]) * weight.astype(jnp.float32)

            @pl.when(last_sends(d))
            def _():
                last_copy(me, mask, last_send_to(d)).start()

            @pl.when(half(col, 4) == y)
            def _():
                put(col, y, val.T)

            @pl.when(jnp.logical_and(on == 1, mask == 1))
            def _():
                put(me, 1 - y, val)

    sum_start(STEPS + 1, [sums[2]])

    @pl.when(on == 1)
    def _():
        for mask, src in ((3, 2), (0, 1), (2, 1)):
            q = sources[src].q
            last_copy(q, jnp.int32(mask), jnp.int32(src)).wait_recv()
            col = other(q, jnp.int32(mask))
            if mask == 3:
                put(q, 1 - y, buf[end, q, col])
            else:
                put(col, 1 - y, buf[end, q, col].T)

    @pl.when(on == 0)
    def _():
        for mask, src in ((5, 4), (4, 1), (7, 6), (6, 1)):
            q = sources[src].q
            last_copy(q, jnp.int32(mask), jnp.int32(src)).wait_recv()
            col = other(q, jnp.int32(mask))
            if src == YN:
                put(col, 1 - y, buf[end, q, col].T)
            else:
                put(q, 1 - y, buf[end, q, col])

    @pl.loop(0, SLOTS)
    def _(d):
        @pl.when(last_sends(d))
        def _():
            last_copy(me, last_mask(d), last_send_to(d)).wait_send()

    (energy,) = sum_finish(STEPS + 1, 1)
    e_ref[0] = 2.0 * jnp.sum(energy)


def solution(mesh):
    n_cols = mesh.shape["col"]

    def local_fn(ham_blk, bounds, n_occ):
        rows_n, cols_n = ham_blk.shape
        n = cols_n * n_cols
        blk_n = n // PANELS
        f32 = jnp.float32
        return pl.pallas_call(
            lambda *refs: kernel(n, *refs),
            out_shape=(jax.ShapeDtypeStruct((rows_n, cols_n), f32), jax.ShapeDtypeStruct((1,), f32)),
            in_specs=[
                pl.BlockSpec(memory_space=pltpu.SMEM),
                pl.BlockSpec(memory_space=pltpu.SMEM),
                pl.BlockSpec(memory_space=pltpu.VMEM),
            ],
            out_specs=(pl.BlockSpec(memory_space=pltpu.VMEM), pl.BlockSpec(memory_space=pltpu.SMEM)),
            scratch_shapes=[
                pltpu.VMEM((2, PANELS, PANELS, blk_n, blk_n), f32),
                pltpu.VMEM((PANELS, blk_n, blk_n), f32),
                pltpu.VMEM((PANELS, blk_n, blk_n), f32),
                pltpu.VMEM((blk_n, blk_n), f32),
                pltpu.VMEM((STEPS + 2, PANELS, 3, 8, 128), f32),
                pltpu.VMEM((8, blk_n), f32),
                pltpu.VMEM((3, 8, 128), f32),
                pltpu.SemaphoreType.DMA((2, PANELS, SLOTS, 3)),
                pltpu.SemaphoreType.DMA((2, PANELS, SLOTS)),
                pltpu.SemaphoreType.DMA((STEPS + 2, PANELS)),
                pltpu.SemaphoreType.DMA((STEPS + 2, PANELS)),
                pltpu.SemaphoreType.DMA((PANELS,)),
                pltpu.SemaphoreType.DMA((PANELS,)),
            ],
            compiler_params=pltpu.CompilerParams(collective_id=0, has_side_effects=True, vmem_limit_bytes=60 << 20),
            name="purify",
        )(bounds, n_occ, ham_blk)

    spec_mat = P(("spin", "row"), "col")
    return jax.shard_map(local_fn, mesh=mesh, in_specs=(spec_mat, P("spin"), P("spin")), out_specs=(spec_mat, P("spin")), check_vma=False)
```

```python
import jax
import jax.numpy as jnp
from jax import lax
from jax.experimental import pallas as pl
from jax.experimental.pallas import tpu as pltpu
from jax.sharding import PartitionSpec as P

STEPS = 3
PANELS = 8
SLOTS = 5
CORNERS = 2
MESH = pl.DeviceIdType.MESH
NN = (((1,), (0,)), ((), ()))
NT = (((1,), (1,)), ((), ()))


def dot(lhs, rhs, dims):
    return lax.dot_general(lhs, rhs, dims, precision=lax.Precision.HIGHEST, preferred_element_type=jnp.float32)


def flag(cond):
    return lax.convert_element_type(cond, jnp.int32)


def pick(index, values):
    return sum(flag(index == k) * v for k, v in enumerate(values) if not (isinstance(v, int) and v == 0))


def half(val, by=2):
    return lax.div(val, jnp.int32(by))


def part(val, by=2):
    return lax.rem(val, jnp.int32(by))


def flip(bit, by):
    return bit + by - 2 * bit * by


def panel_bits(q):
    return q // 4, q % 2, (q // 2) % 2


def packed(digits, base):
    return sum(d * base**k for k, d in enumerate(digits))


def h_blocks(q):
    x, y, c = panel_bits(q)
    if x == y:
        local = {
            (0, 0): ((1, 0), (3, 0), (2, 0), (0, 0), (1, 1)),
            (0, 1): ((3, 0), (1, 0), (1, 1), (2, 0), (3, 1)),
            (1, 0): ((1, 0), (2, 0), (3, 0), (0, 0), (1, 1)),
            (1, 1): ((3, 0), (1, 0), (1, 1), (2, 0), (3, 1)),
        }[x, c]
    else:
        local = tuple((2 * k + (b + y) % 2, b) for b in range(2) for k in range(2))
    return tuple((4 * y + a, 4 * x + 2 * c + b) for a, b in local)


def x_blocks(q):
    x, y, c = panel_bits(q)
    return tuple(q ^ m for m in (4 + 2 * x, 1 + 2 * y, 5 + 2 * y, 0, 2, 7 - 2 * y))


def kernel(n, bounds, n_occ, h_ref, out_ref, e_ref, buf, hrow, x2row, acc, parts, coef, sums, send_sem, recv_sem, part_send, part_recv, last_send, last_recv):
    blk_n = n // PANELS
    y = lax.axis_index("row")
    j = lax.axis_index("col")
    x, c = half(j), part(j)
    me = 4 * x + 2 * c + y
    on = 1 - flip(x, y)

    class Source:
        def __init__(self, q, h_pack, h_count, x_pack, x_count):
            self.fields = q, h_pack, h_count, x_pack, x_count
            self.q, self.h_pack, self.h_count, self.x_pack, self.x_count = self.fields

        def __add__(self, other):
            return Source(*(a + b for a, b in zip(self.fields, other.fields)))

        def __mul__(self, by):
            return Source(*(a * by for a in self.fields))

    def device(mask):
        dx, dy, dc = flip(x, half(mask, 4)), flip(y, part(mask)), flip(c, part(half(mask)))
        return (0, dy, 2 * dx + dc)

    def source(mask):
        q = panel(mask)
        return Source(
            q,
            pick(q, [packed([8 * row + col for row, col in h_blocks(k)], 64) for k in range(PANELS)]),
            pick(q, [len(h_blocks(k)) for k in range(PANELS)]),
            pick(q, [packed(x_blocks(k), 8) for k in range(PANELS)]),
            pick(q, [5 - (k // 2) % 2 for k in range(PANELS)]),
        )

    def panel(mask):
        return 4 * flip(x, mask // 4) + 2 * flip(c, (mask // 2) % 2) + flip(y, mask % 2)

    def h_place(src, t):
        code = part(lax.div(src.h_pack, pick(t, [64**k for k in range(SLOTS)])), 64)
        return half(code, 8), part(code, 8)

    def x_place(src, t):
        return src.q, part(lax.div(src.x_pack, pick(t, [8**k for k in range(SLOTS + 1)])), 8)

    devices = [device(jnp.int32(mask)) for mask in range(8)]
    sources = [source(mask) for mask in range(8)]

    PARTNER, XN, YN, DIAG = 2, 4, 1, 5

    barrier = pltpu.get_barrier_semaphore()
    for mask in range(1, 8):
        pl.semaphore_signal(barrier, inc=1, device_id=devices[mask], device_id_type=MESH)
    pl.semaphore_wait(barrier, 7)

    class Exchange:
        def __init__(self, rnd, buf_id, place, count, own_src=None):
            self.rnd, self.buf_id, self.place, self.count = rnd, buf_id, place, count
            self.own_src = own_src or (lambda row, col: buf.at[buf_id, row, col])

        def copy(self, at, t, way, view, src=None):
            q, row, col, _ = at
            block = view(buf.at[self.buf_id, row, col])
            return pltpu.make_async_remote_copy(
                src_ref=block if src is None else view(src),
                dst_ref=block,
                send_sem=send_sem.at[self.rnd % 2, q, t, way],
                recv_sem=recv_sem.at[self.rnd % 2, q, t],
                device_id=devices[(PARTNER, XN, YN)[way]],
                device_id_type=MESH,
            )

        def pieces(self, at, t, body):
            mid = blk_n // 2

            @pl.when(at[1] != at[2])
            def _():
                body(t, lambda ref: ref, flag(t == 0) + flag(t == 2))

            @pl.when(at[1] == at[2])
            def _():
                body(t, lambda ref: ref.at[pl.ds(0, mid), :], jnp.int32(0))
                body(t + CORNERS, lambda ref: ref.at[pl.ds(mid, mid), pl.ds(mid, mid)], flag(t == 4))

        def own(self, at, t, act):
            def body(slot, view, x_way):
                for way in range(3):
                    act(self.copy(at, slot, way, view, self.own_src(*at[1:3])))

            self.pieces(at, t, body)

        def forward(self, mask, at, t, act):
            def body(slot, view, x_way):
                act(self.copy(at, slot, 0, view))
                if mask == XN:

                    @pl.when(x_way == 1)
                    def _():
                        act(self.copy(at, slot, 2, view))

                if mask == YN:

                    @pl.when(x_way == 0)
                    def _():
                        act(self.copy(at, slot, 1, view))

            self.pieces(at, t, body)

        def forward_any(self, k, masks, at, t, act):
            for mask in (XN, YN, DIAG):
                if mask in masks:

                    @pl.when(k == masks.index(mask))
                    def _():
                        self.forward(mask, at, t, act)

        def arrive(self, k, masks, at, t):
            self.pieces(at, t, lambda slot, view, x_way: self.copy(at, slot, 0, view).wait_recv())
            self.forward_any(k, masks, at, t, lambda copy: copy.start())
            mid = blk_n // 2

            @pl.when(at[1] == at[2])
            def _():
                block = buf.at[self.buf_id, at[1], at[2]]
                block[mid:, :mid] = block[:mid, mid:].T

        def at(self, src, t):
            return (src.q, *self.place(src, t), src)

        def each(self, masks, body, first=0, last=SLOTS):
            srcs = [mask if isinstance(mask, Source) else sources[mask] for mask in masks]
            many = len(srcs)

            @pl.loop(0, (last - first) * many)
            def _(i):
                t, k = first + half(i, many), part(i, many)
                src = srcs[0] if many == 1 else Source(*(pick(k, vals) for vals in zip(*(src.fields for src in srcs))))

                @pl.when(t < self.count(src))
                def _():
                    body(k, self.at(src, t), t)

        def drain(self):
            self.each((0,), lambda k, at, t: self.own(at, t, lambda copy: copy.wait_send()))
            far = (XN, YN, DIAG)
            self.each(far, lambda k, at, t: self.forward_any(k, far, at, t, lambda copy: copy.wait_send()))

    def part_copy(rnd, src, mask):
        return pltpu.make_async_remote_copy(
            src_ref=parts.at[rnd, src],
            dst_ref=parts.at[rnd, src],
            send_sem=part_send.at[rnd, mask],
            recv_sem=part_recv.at[rnd, src],
            device_id=devices[mask],
            device_id_type=MESH,
        )

    def sum_start(rnd, vals):
        for k, val in enumerate(vals):
            parts[rnd, me, k : k + 1] = jnp.sum(val, axis=0, keepdims=True)
        for mask in range(1, 8):
            part_copy(rnd, me, mask).start()

    def sum_finish(rnd, count):
        for mask in range(1, 8):
            part_copy(rnd, sources[mask].q, mask).wait_recv()
        for mask in range(1, 8):
            part_copy(rnd, me, mask).wait_send()
        tot = parts[rnd, 0]
        for q in range(1, PANELS):
            tot = tot + parts[rnd, q]
        return [jnp.sum(tot[k : k + 1], axis=1, keepdims=True) for k in range(count)]

    def fold(val):
        rows, cols = val.shape
        val = jnp.sum(val.reshape(rows // 8, 8, cols), axis=0)
        tot = val[:, :128]
        for k in range(1, cols // 128):
            tot = tot + val[:, k * 128 : (k + 1) * 128]
        return tot

    def span(k):
        return pl.ds(pl.multiple_of(k * blk_n, blk_n), blk_n)

    def clear():
        @pl.loop(0, PANELS)
        def _(col):
            x2row[col] = jnp.zeros((blk_n, blk_n), jnp.float32)

    def h_src(row, col):
        return h_ref.at[span(row - 4 * y), span(col - 2 * j)]

    hx = Exchange(0, 1, h_place, lambda src: src.h_count, h_src)
    hx.each((0,), lambda k, at, t: hx.own(at, t, lambda copy: copy.start()))

    rows_n, cols_n = h_ref.shape
    mu_part = jnp.zeros((8, 128), jnp.float32)
    for k in range(rows_n // blk_n):
        tile = h_ref[k * blk_n : (k + 1) * blk_n, :]
        row_ids = y * rows_n + k * blk_n + lax.broadcasted_iota(jnp.int32, tile.shape, 0)
        col_ids = j * cols_n + lax.broadcasted_iota(jnp.int32, tile.shape, 1)
        mu_part = mu_part + fold(jnp.where(row_ids == col_ids, tile, 0.0))
    sum_start(0, [mu_part])
    clear()

    eye = (lax.broadcasted_iota(jnp.int32, (blk_n, blk_n), 0) == lax.broadcasted_iota(jnp.int32, (blk_n, blk_n), 1)).astype(jnp.float32)
    (trace_h,) = sum_finish(0, 1)
    occ = n_occ[0].astype(jnp.float32)
    mu = trace_h / n
    lam = jnp.minimum(occ / (bounds[1] - mu), (n - occ) / (mu - bounds[0]))
    coef[0:1, :] = jnp.broadcast_to(lam / n, (1, blk_n))
    coef[1:2, :] = jnp.broadcast_to(mu, (1, blk_n))
    coef[2:3, :] = jnp.broadcast_to(jnp.full((1, 1), occ / n, jnp.float32), (1, blk_n))

    def first_x(own, at):
        _, row, col = at[:3]
        blk = h_src(row, col)[...] if own else buf[1, row, col]
        diag = eye * (row == col).astype(jnp.float32)
        val = coef[0:1, :] * (coef[1:2, :] * diag - blk) + coef[2:3, :] * diag
        buf[0, row, col] = val

        @pl.when(row != col)
        def _():
            buf[0, col, row] = val.T

        @pl.when(row == me)
        def _():
            hrow[col] = blk

        @pl.when(jnp.logical_and(col == me, row != me))
        def _():
            hrow[row] = blk.T

    def use(b, row, col):
        blk = buf[b, row, col]
        x2row[col] += dot(buf[b, me, row], blk, NN)
        x2row[row] += dot(buf[b, me, col], blk, NT)
        buf[b, col, row] = blk.T

    def use_pair(b, row, col):
        blk = [buf[b, row, k] for k in col]
        left = buf[b, me, row]
        right = [buf[b, me, k] for k in col]
        for k in range(2):
            x2row[col[k]] += dot(left, blk[k], NN)
        x2row[row] += dot(right[0], blk[0], NT) + dot(right[1], blk[1], NT)
        for k in range(2):
            buf[b, col[k], row] = blk[k].T

    def use_diag(b, row, col):
        blk, mid = buf[b, row, col], buf[b, row, row]
        left = buf[b, me, row]
        right = buf[b, me, col]
        x2row[col] += dot(left, blk, NN)
        x2row[row] += dot(right, blk, NT) + dot(left, mid, NN)
        buf[b, col, row] = blk.T

    def h_take(masks):
        def body(k, at, t):
            hx.arrive(k, masks, at, t)
            first_x(False, at)

        return body

    def h_unit(col, kind):
        cross = half(kind)
        first = 4 * flip(half(col, 4), cross) + (1 - cross) * 2 * kind + cross * flip(part(col), part(kind))
        second = first + 1 + cross
        x2row[col] += dot(buf[0, me, first], buf[0, first, col], NN) + dot(buf[0, me, second], buf[0, second, col], NN)

    @pl.loop(0, 4)
    def _(k):
        first_x(True, (me, 4 * y + k, me))

    hx.each((0,), lambda k, at, t: first_x(True, at))
    hx.each((PARTNER,), h_take((PARTNER,)))

    near = (XN, YN, XN + 2, YN + 2)
    far = (DIAG, DIAG + 2)
    off = 1 - on
    hx.each(near, h_take(near), 0, 1)

    @pl.loop(0, 4 + 4 * on)
    def _(i):
        h_unit(on * (4 * y + half(i)) + off * (4 - 4 * y + i), on * part(i) + off * (2 + y))

    hx.each(near, h_take(near), 1, SLOTS)

    @pl.loop(0, 16)
    def _(i):
        h_unit(on * (4 * flip(y, half(i, 8)) + half(part(i, 8))) + off * half(i), on * 2 + part(i))

    @pl.loop(0, 4 * off)
    def _(i):
        h_unit(4 * y + i, 2 + y)

    hx.each(far, h_take(far))

    @pl.loop(0, 8)
    def _(i):
        h_unit(on * (4 - 4 * y + half(i)) + off * i, on * part(i) + off * (3 - y))

    def product(old, col):
        tot = dot(x2row[0], buf[old, 0, col], NN)
        for k in range(1, PANELS):
            tot = tot + dot(x2row[k], buf[old, k, col], NN)
        return tot

    def traces(old, rnd):
        t1 = fold(buf[old, me, me] * eye)
        sums[...] = jnp.zeros_like(sums)

        @pl.loop(0, PANELS)
        def _(col):
            xv = buf[old, me, col]
            sums[0] += fold(xv * xv)
            sums[1] += fold(xv * x2row[col])

        sum_start(rnd, [t1, sums[0], sums[1]])

    def mix(rnd):
        t1, t2, t3 = sum_finish(rnd, 3)
        cval = (t2 - t3) / (t1 - t2)
        inv = 1.0 / (1.0 - cval)
        for k, val in enumerate(((1.0 - 2.0 * cval) * inv, (1.0 + cval) * inv, inv)):
            coef[k : k + 1, :] = jnp.broadcast_to(val, (1, blk_n))

    def updated(old, col):
        return coef[0:1, :] * buf[old, me, col] + coef[1:2, :] * x2row[col] - coef[2:3, :] * acc[...]

    before = hx
    for step in range(STEPS - 1):
        old, new = step % 2, (step + 1) % 2
        before.drain()
        traces(old, 1 + step)
        ex = Exchange(1 + step, new, x_place, lambda src: src.x_count)

        @pl.loop(0, SLOTS + 1)
        def _(t):
            at = ex.at(sources[0], t)
            col = at[2]
            acc[...] = product(old, col)

            @pl.when(t == 0)
            def _():
                mix(1 + step)

            buf[new, me, col] = updated(old, col)

            @pl.when(t < sources[0].x_count)
            def _():
                ex.own(at, t, lambda copy: copy.start())

        clear()

        def x_take(masks):
            def body(k, at, t):
                ex.arrive(k, masks, at, t)
                _, row, col = at[:3]

                @pl.when(col == me)
                def _():
                    buf[new, me, row] = buf[new, row, col].T

            return body

        def x_first(k, at, t):
            src = at[3]
            use_pair(new, at[1], (at[2], x_place(src, 1)[1]))

        def x_second(k, at, t):
            use_diag(new, at[1], at[2])

        def x_last(k, at, t):
            use(new, at[1], at[2])

        near = (PARTNER, XN, YN, XN + 2, YN + 2)
        far = (DIAG, DIAG + 2)
        ex.each((0,), x_first, 0, 1)
        ex.each(near, x_take(near), 0, 2)
        ex.each(near, x_first, 0, 1)
        ex.each(near, x_take(near), 2, 4)
        ex.each((0, *near), x_second, 2, 3)
        ex.each(near, x_take(near), 4, 5)
        ex.each((0, *near), x_last, 4, 5)
        ex.each(far, x_take(far), 0, 2)
        ex.each(far, x_first, 0, 1)
        ex.each(far, x_take(far), 2, 4)
        ex.each(far, x_second, 2, 3)
        ex.each(far, x_take(far), 4, 5)
        ex.each(far, x_last, 4, 5)
        before = ex

    old, end = (STEPS - 1) % 2, STEPS % 2
    before.drain()
    traces(old, STEPS)
    sums[2] = jnp.zeros((8, 128), jnp.float32)

    def other(q, mask):
        return 4 * flip(half(q, 4), half(mask, 4)) + 2 * flip(part(half(q)), part(half(mask))) + flip(part(q), part(mask))

    def last_copy(q, mask, to):
        block = buf.at[end, q, other(q, mask)]
        return pltpu.make_async_remote_copy(
            src_ref=block,
            dst_ref=block,
            send_sem=last_send.at[mask],
            recv_sem=last_recv.at[mask],
            device_id=device(to),
            device_id_type=MESH,
        )

    def put(row, b, val):
        out_ref[span(row - 4 * y), span(b)] = val

    def last_mask(d):
        return on * pick(d, (5, 4, 7, 6, 3, 0, 1, 2)) + (1 - on) * pick(d, (0, 2, 4, 5, 6, 7, 1, 3))

    def last_send_to(d):
        return on * pick(d, (4, 1, 6, 1, 2)) + (1 - on)

    def last_sends(d):
        return d < 2 + 3 * on

    @pl.loop(0, PANELS)
    def _(d):
        @pl.when(d < 6 + 2 * on)
        def _():
            mask = last_mask(d)
            col = other(me, mask)
            acc[...] = product(old, col)

            @pl.when(d == 0)
            def _():
                mix(STEPS)

            val = updated(old, col)

            @pl.when(last_sends(d))
            def _():
                buf[end, me, col] = val

            weight = 1 + on * part(mask) * (1 - half(mask, 4))
            sums[2] += fold(val * hrow[col]) * weight.astype(jnp.float32)

            @pl.when(last_sends(d))
            def _():
                last_copy(me, mask, last_send_to(d)).start()

            @pl.when(half(col, 4) == y)
            def _():
                put(col, y, val.T)

            @pl.when(jnp.logical_and(on == 1, mask == 1))
            def _():
                put(me, 1 - y, val)

    sum_start(STEPS + 1, [sums[2]])

    @pl.when(on == 1)
    def _():
        for mask, src in ((3, 2), (0, 1), (2, 1)):
            q = sources[src].q
            last_copy(q, jnp.int32(mask), jnp.int32(src)).wait_recv()
            col = other(q, jnp.int32(mask))
            if mask == 3:
                put(q, 1 - y, buf[end, q, col])
            else:
                put(col, 1 - y, buf[end, q, col].T)

    @pl.when(on == 0)
    def _():
        for mask, src in ((5, 4), (4, 1), (7, 6), (6, 1)):
            q = sources[src].q
            last_copy(q, jnp.int32(mask), jnp.int32(src)).wait_recv()
            col = other(q, jnp.int32(mask))
            if src == YN:
                put(col, 1 - y, buf[end, q, col].T)
            else:
                put(q, 1 - y, buf[end, q, col])

    @pl.loop(0, SLOTS)
    def _(d):
        @pl.when(last_sends(d))
        def _():
            last_copy(me, last_mask(d), last_send_to(d)).wait_send()

    (energy,) = sum_finish(STEPS + 1, 1)
    e_ref[0] = 2.0 * jnp.sum(energy)


def solution(mesh):
    n_cols = mesh.shape["col"]

    def local_fn(ham_blk, bounds, n_occ):
        rows_n, cols_n = ham_blk.shape
        n = cols_n * n_cols
        blk_n = n // PANELS
        f32 = jnp.float32
        return pl.pallas_call(
            lambda *refs: kernel(n, *refs),
            out_shape=(jax.ShapeDtypeStruct((rows_n, cols_n), f32), jax.ShapeDtypeStruct((1,), f32)),
            in_specs=[
                pl.BlockSpec(memory_space=pltpu.SMEM),
                pl.BlockSpec(memory_space=pltpu.SMEM),
                pl.BlockSpec(memory_space=pltpu.VMEM),
            ],
            out_specs=(pl.BlockSpec(memory_space=pltpu.VMEM), pl.BlockSpec(memory_space=pltpu.SMEM)),
            scratch_shapes=[
                pltpu.VMEM((2, PANELS, PANELS, blk_n, blk_n), f32),
                pltpu.VMEM((PANELS, blk_n, blk_n), f32),
                pltpu.VMEM((PANELS, blk_n, blk_n), f32),
                pltpu.VMEM((blk_n, blk_n), f32),
                pltpu.VMEM((STEPS + 2, PANELS, 8, 128), f32),
                pltpu.VMEM((8, blk_n), f32),
                pltpu.VMEM((3, 8, 128), f32),
                pltpu.SemaphoreType.DMA((2, PANELS, SLOTS + CORNERS, 3)),
                pltpu.SemaphoreType.DMA((2, PANELS, SLOTS + CORNERS)),
                pltpu.SemaphoreType.DMA((STEPS + 2, PANELS)),
                pltpu.SemaphoreType.DMA((STEPS + 2, PANELS)),
                pltpu.SemaphoreType.DMA((PANELS,)),
                pltpu.SemaphoreType.DMA((PANELS,)),
            ],
            compiler_params=pltpu.CompilerParams(collective_id=0, has_side_effects=True, vmem_limit_bytes=48 << 20),
            name="purify",
        )(bounds, n_occ, ham_blk)

    spec_mat = P(("spin", "row"), "col")
    return jax.shard_map(local_fn, mesh=mesh, in_specs=(spec_mat, P("spin"), P("spin")), out_specs=(spec_mat, P("spin")), check_vma=False)
```

```python
import jax
import jax.numpy as jnp
from jax import lax
from jax.experimental import pallas as pl
from jax.experimental.pallas import tpu as pltpu
from jax.sharding import PartitionSpec as P

STEPS = 3
PANELS = 8
SLOTS = 5
CORNERS = 2
MESH = pl.DeviceIdType.MESH
NN = (((1,), (0,)), ((), ()))
NT = (((1,), (1,)), ((), ()))


def dot(lhs, rhs, dims):
    return lax.dot_general(lhs, rhs, dims, precision=lax.Precision.HIGHEST, preferred_element_type=jnp.float32)


def flag(cond):
    return lax.convert_element_type(cond, jnp.int32)


def pick(index, values):
    return sum(flag(index == k) * v for k, v in enumerate(values) if not (isinstance(v, int) and v == 0))


def half(val, by=2):
    return lax.div(val, jnp.int32(by))


def part(val, by=2):
    return lax.rem(val, jnp.int32(by))


def flip(bit, by):
    return bit + by - 2 * bit * by


def panel_bits(q):
    return q // 4, q % 2, (q // 2) % 2


def packed(digits, base):
    return sum(d * base**k for k, d in enumerate(digits))


def h_blocks(q):
    x, y, c = panel_bits(q)
    if x == y:
        local = {
            (0, 0): ((1, 0), (3, 0), (2, 0), (0, 0), (1, 1)),
            (0, 1): ((3, 0), (1, 0), (1, 1), (2, 0), (3, 1)),
            (1, 0): ((1, 0), (2, 0), (3, 0), (0, 0), (1, 1)),
            (1, 1): ((3, 0), (1, 0), (1, 1), (2, 0), (3, 1)),
        }[x, c]
    else:
        local = tuple((2 * k + (b + y) % 2, b) for b in range(2) for k in range(2))
    return tuple((4 * y + a, 4 * x + 2 * c + b) for a, b in local)


def x_blocks(q):
    x, y, c = panel_bits(q)
    return tuple(q ^ m for m in (4 + 2 * x, 1 + 2 * y, 5 + 2 * y, 0, 2, 7 - 2 * y))


def kernel(n, bounds, n_occ, h_hbm, out_ref, e_ref, h_ref, h_sem, buf, hrow, x2row, acc, parts, coef, sums, send_sem, recv_sem, part_send, part_recv, last_send, last_recv):
    blk_n = n // PANELS
    y = lax.axis_index("row")
    j = lax.axis_index("col")
    x, c = half(j), part(j)
    me = 4 * x + 2 * c + y
    on = 1 - flip(x, y)

    class Source:
        def __init__(self, q, h_pack, h_count, x_pack, x_count):
            self.fields = q, h_pack, h_count, x_pack, x_count
            self.q, self.h_pack, self.h_count, self.x_pack, self.x_count = self.fields

        def __add__(self, other):
            return Source(*(a + b for a, b in zip(self.fields, other.fields)))

        def __mul__(self, by):
            return Source(*(a * by for a in self.fields))

    def device(mask):
        dx, dy, dc = flip(x, half(mask, 4)), flip(y, part(mask)), flip(c, part(half(mask)))
        return (0, dy, 2 * dx + dc)

    def source(mask):
        q = panel(mask)
        return Source(
            q,
            pick(q, [packed([8 * row + col for row, col in h_blocks(k)], 64) for k in range(PANELS)]),
            pick(q, [len(h_blocks(k)) for k in range(PANELS)]),
            pick(q, [packed(x_blocks(k), 8) for k in range(PANELS)]),
            pick(q, [5 - (k // 2) % 2 for k in range(PANELS)]),
        )

    def panel(mask):
        return 4 * flip(x, mask // 4) + 2 * flip(c, (mask // 2) % 2) + flip(y, mask % 2)

    def h_place(src, t):
        code = part(lax.div(src.h_pack, pick(t, [64**k for k in range(SLOTS)])), 64)
        return half(code, 8), part(code, 8)

    def x_place(src, t):
        return src.q, part(lax.div(src.x_pack, pick(t, [8**k for k in range(SLOTS + 1)])), 8)

    def x_at(src, t):
        return src.q, src.q, part(half(src.x_pack, 8**t), 8), src

    devices = [device(jnp.int32(mask)) for mask in range(8)]
    sources = [source(mask) for mask in range(8)]

    PARTNER, XN, YN, DIAG = 2, 4, 1, 5

    h_in = pltpu.make_async_copy(h_hbm, h_ref, h_sem)
    h_in.start()

    barrier = pltpu.get_barrier_semaphore()
    for mask in range(1, 8):
        pl.semaphore_signal(barrier, inc=1, device_id=devices[mask], device_id_type=MESH)
    pl.semaphore_wait(barrier, 7)
    h_in.wait()

    class Exchange:
        def __init__(self, rnd, buf_id, place, count, own_src=None):
            self.rnd, self.buf_id, self.place, self.count = rnd, buf_id, place, count
            self.own_src = own_src or (lambda row, col: buf.at[buf_id, row, col])

        def copy(self, at, t, way, view, src=None):
            q, row, col, _ = at
            block = view(buf.at[self.buf_id, row, col])
            return pltpu.make_async_remote_copy(
                src_ref=block if src is None else view(src),
                dst_ref=block,
                send_sem=send_sem.at[self.rnd % 2, q, t, way],
                recv_sem=recv_sem.at[self.rnd % 2, q, t],
                device_id=devices[(PARTNER, XN, YN)[way]],
                device_id_type=MESH,
            )

        def pieces(self, at, t, body):
            mid = blk_n // 2

            @pl.when(at[1] != at[2])
            def _():
                body(t, lambda ref: ref, flag(t == 0) + flag(t == 2))

            @pl.when(at[1] == at[2])
            def _():
                body(t, lambda ref: ref.at[pl.ds(0, mid), :], jnp.int32(0))
                body(t + CORNERS, lambda ref: ref.at[pl.ds(mid, mid), pl.ds(mid, mid)], flag(t == 4))

        def own(self, at, t, act):
            def body(slot, view, x_way):
                for way in range(3):
                    act(self.copy(at, slot, way, view, self.own_src(*at[1:3])))

            self.pieces(at, t, body)

        def forward(self, mask, at, t, act):
            def body(slot, view, x_way):
                act(self.copy(at, slot, 0, view))
                if mask == XN:

                    @pl.when(x_way == 1)
                    def _():
                        act(self.copy(at, slot, 2, view))

                if mask == YN:

                    @pl.when(x_way == 0)
                    def _():
                        act(self.copy(at, slot, 1, view))

            self.pieces(at, t, body)

        def forward_any(self, k, masks, at, t, act):
            for mask in (XN, YN, DIAG):
                if mask in masks:

                    @pl.when(k == masks.index(mask))
                    def _():
                        self.forward(mask, at, t, act)

        def arrive(self, k, masks, at, t):
            self.pieces(at, t, lambda slot, view, x_way: self.copy(at, slot, 0, view).wait_recv())
            self.forward_any(k, masks, at, t, lambda copy: copy.start())
            mid = blk_n // 2

            @pl.when(at[1] == at[2])
            def _():
                block = buf.at[self.buf_id, at[1], at[2]]
                block[mid:, :mid] = block[:mid, mid:].T

        def take(self, mask, at, t):
            mid = blk_n // 2
            views = [(t, lambda ref: ref)]
            if t == 3:
                views = [(t, lambda ref: ref.at[pl.ds(0, mid), :]), (t + CORNERS, lambda ref: ref.at[pl.ds(mid, mid), pl.ds(mid, mid)])]
            for slot, view in views:
                self.copy(at, slot, 0, view).wait_recv()
            for slot, view in views:
                if mask in (XN, YN, DIAG):
                    self.copy(at, slot, 0, view).start()
                if mask == XN and t in (0, 2):
                    self.copy(at, slot, 2, view).start()
                if mask == YN and t not in (0, 2):
                    self.copy(at, slot, 1, view).start()
            if t == 3:
                block = buf.at[self.buf_id, at[1], at[2]]
                block[mid:, :mid] = block[:mid, mid:].T

        def at(self, src, t):
            return (src.q, *self.place(src, t), src)

        def each(self, masks, body, first=0, last=SLOTS):
            srcs = [mask if isinstance(mask, Source) else sources[mask] for mask in masks]
            many = len(srcs)

            @pl.loop(0, (last - first) * many)
            def _(i):
                t, k = first + half(i, many), part(i, many)
                src = srcs[0] if many == 1 else Source(*(pick(k, vals) for vals in zip(*(src.fields for src in srcs))))

                @pl.when(t < self.count(src))
                def _():
                    body(k, self.at(src, t), t)

        def drain(self):
            self.each((0,), lambda k, at, t: self.own(at, t, lambda copy: copy.wait_send()))
            far = (XN, YN, DIAG)
            self.each(far, lambda k, at, t: self.forward_any(k, far, at, t, lambda copy: copy.wait_send()))

    def part_copy(rnd, src, mask):
        return pltpu.make_async_remote_copy(
            src_ref=parts.at[rnd, src],
            dst_ref=parts.at[rnd, src],
            send_sem=part_send.at[rnd, mask],
            recv_sem=part_recv.at[rnd, src],
            device_id=devices[mask],
            device_id_type=MESH,
        )

    def sum_start(rnd, vals):
        for k, val in enumerate(vals):
            parts[rnd, me, k : k + 1] = jnp.sum(val, axis=0, keepdims=True)
        for mask in range(1, 8):
            part_copy(rnd, me, mask).start()

    def sum_finish(rnd, count):
        for mask in range(1, 8):
            part_copy(rnd, sources[mask].q, mask).wait_recv()
        for mask in range(1, 8):
            part_copy(rnd, me, mask).wait_send()
        tot = parts[rnd, 0]
        for q in range(1, PANELS):
            tot = tot + parts[rnd, q]
        return [jnp.sum(tot[k : k + 1], axis=1, keepdims=True) for k in range(count)]

    def fold(val):
        rows, cols = val.shape
        val = jnp.sum(val.reshape(rows // 8, 8, cols), axis=0)
        tot = val[:, :128]
        for k in range(1, cols // 128):
            tot = tot + val[:, k * 128 : (k + 1) * 128]
        return tot

    def span(k):
        return pl.ds(pl.multiple_of(k * blk_n, blk_n), blk_n)

    def clear():
        @pl.loop(0, PANELS)
        def _(col):
            x2row[col] = jnp.zeros((blk_n, blk_n), jnp.float32)

    def h_src(row, col):
        return h_ref.at[span(row - 4 * y), span(col - 2 * j)]

    hx = Exchange(0, 1, h_place, lambda src: src.h_count, h_src)
    hx.each((0,), lambda k, at, t: hx.own(at, t, lambda copy: copy.start()))

    rows_n, cols_n = h_ref.shape
    mu_part = jnp.zeros((8, 128), jnp.float32)
    for k in range(rows_n // blk_n):
        tile = h_ref[k * blk_n : (k + 1) * blk_n, :]
        row_ids = y * rows_n + k * blk_n + lax.broadcasted_iota(jnp.int32, tile.shape, 0)
        col_ids = j * cols_n + lax.broadcasted_iota(jnp.int32, tile.shape, 1)
        mu_part = mu_part + fold(jnp.where(row_ids == col_ids, tile, 0.0))
    sum_start(0, [mu_part])
    clear()

    eye = (lax.broadcasted_iota(jnp.int32, (blk_n, blk_n), 0) == lax.broadcasted_iota(jnp.int32, (blk_n, blk_n), 1)).astype(jnp.float32)
    (trace_h,) = sum_finish(0, 1)
    occ = n_occ[0].astype(jnp.float32)
    mu = trace_h / n
    lam = jnp.minimum(occ / (bounds[1] - mu), (n - occ) / (mu - bounds[0]))
    coef[0:1, :] = jnp.broadcast_to(lam / n, (1, blk_n))
    coef[1:2, :] = jnp.broadcast_to(mu, (1, blk_n))
    coef[2:3, :] = jnp.broadcast_to(jnp.full((1, 1), occ / n, jnp.float32), (1, blk_n))

    def first_x(own, at):
        _, row, col = at[:3]
        blk = h_src(row, col)[...] if own else buf[1, row, col]
        diag = eye * (row == col).astype(jnp.float32)
        val = coef[0:1, :] * (coef[1:2, :] * diag - blk) + coef[2:3, :] * diag
        buf[0, row, col] = val

        @pl.when(row != col)
        def _():
            buf[0, col, row] = val.T

        @pl.when(row == me)
        def _():
            hrow[col] = blk

        @pl.when(jnp.logical_and(col == me, row != me))
        def _():
            hrow[row] = blk.T

    def use(b, row, col):
        blk = buf[b, row, col]
        x2row[col] += dot(buf[b, me, row], blk, NN)
        x2row[row] += dot(buf[b, me, col], blk, NT)
        buf[b, col, row] = blk.T

    def use_pair(b, row, col):
        blk = [buf[b, row, k] for k in col]
        left = buf[b, me, row]
        right = [buf[b, me, k] for k in col]
        for k in range(2):
            x2row[col[k]] += dot(left, blk[k], NN)
        x2row[row] += dot(right[0], blk[0], NT) + dot(right[1], blk[1], NT)
        for k in range(2):
            buf[b, col[k], row] = blk[k].T

    def use_diag(b, row, col):
        blk, mid = buf[b, row, col], buf[b, row, row]
        left = buf[b, me, row]
        right = buf[b, me, col]
        x2row[col] += dot(left, blk, NN)
        x2row[row] += dot(right, blk, NT) + dot(left, mid, NN)
        buf[b, col, row] = blk.T

    def h_take(masks):
        def body(k, at, t):
            hx.arrive(k, masks, at, t)
            first_x(False, at)

        return body

    def h_unit(col, kind):
        cross = half(kind)
        first = 4 * flip(half(col, 4), cross) + (1 - cross) * 2 * kind + cross * flip(part(col), part(kind))
        second = first + 1 + cross
        x2row[col] += dot(buf[0, me, first], buf[0, first, col], NN) + dot(buf[0, me, second], buf[0, second, col], NN)

    @pl.loop(0, 4)
    def _(k):
        first_x(True, (me, 4 * y + k, me))

    hx.each((0,), lambda k, at, t: first_x(True, at))
    hx.each((PARTNER,), h_take((PARTNER,)))

    near = (XN, YN, XN + 2, YN + 2)
    far = (DIAG, DIAG + 2)
    off = 1 - on
    hx.each(near, h_take(near), 0, 1)

    @pl.loop(0, 4 + 4 * on)
    def _(i):
        h_unit(on * (4 * y + half(i)) + off * (4 - 4 * y + i), on * part(i) + off * (2 + y))

    hx.each(near, h_take(near), 1, 3)

    @pl.loop(0, 4 * off)
    def _(i):
        h_unit(4 * y + i, 1 - half(i))

    hx.each(near, h_take(near), 3, SLOTS)

    @pl.loop(0, 16)
    def _(i):
        col, kind = on * (4 * flip(y, half(i, 8)) + half(part(i, 8))) + off * half(i), on * 2 + part(i)

        @pl.when(on + flag(half(col, 4) != y) + flag(kind == half(part(col, 4))) > 0)
        def _():
            h_unit(col, kind)

    @pl.loop(0, 4 * off)
    def _(i):
        h_unit(4 * y + i, 2 + y)

    hx.each(far, h_take(far), 0, 2)

    @pl.loop(0, 4 * off)
    def _(i):
        late_half = half(i)
        h_unit(4 * flip(y, late_half) + 2 * part(i) + late_half * (1 - y), 3 - y)

    hx.each(far, h_take(far), 2, SLOTS)

    @pl.loop(0, 4 + 4 * on)
    def _(i):
        late_half = half(i)
        h_unit(on * (4 - 4 * y + half(i)) + off * (4 * flip(y, late_half) + 2 * part(i) + 1 - late_half * (1 - y)), on * part(i) + off * (3 - y))

    def product(old, col):
        tot = dot(x2row[0], buf[old, 0, col], NN)
        for k in range(1, PANELS):
            tot = tot + dot(x2row[k], buf[old, k, col], NN)
        return tot

    def traces(old, rnd):
        t1 = fold(buf[old, me, me] * eye)
        sums[...] = jnp.zeros_like(sums)

        @pl.loop(0, PANELS)
        def _(col):
            xv = buf[old, me, col]
            sums[0] += fold(xv * xv)
            sums[1] += fold(xv * x2row[col])

        sum_start(rnd, [t1, sums[0], sums[1]])

    def mix(rnd):
        t1, t2, t3 = sum_finish(rnd, 3)
        cval = (t2 - t3) / (t1 - t2)
        inv = 1.0 / (1.0 - cval)
        for k, val in enumerate(((1.0 - 2.0 * cval) * inv, (1.0 + cval) * inv, inv)):
            coef[k : k + 1, :] = jnp.broadcast_to(val, (1, blk_n))

    def updated(old, col):
        return coef[0:1, :] * buf[old, me, col] + coef[1:2, :] * x2row[col] - coef[2:3, :] * acc[...]

    before = hx
    for step in range(STEPS - 1):
        old, new = step % 2, (step + 1) % 2
        before.drain()
        traces(old, 1 + step)
        ex = Exchange(1 + step, new, x_place, lambda src: src.x_count)

        @pl.loop(0, SLOTS + 1)
        def _(t):
            at = ex.at(sources[0], t)
            col = at[2]
            acc[...] = product(old, col)

            @pl.when(t == 0)
            def _():
                mix(1 + step)

            buf[new, me, col] = updated(old, col)

            @pl.when(t < sources[0].x_count)
            def _():
                ex.own(at, t, lambda copy: copy.start())

        clear()

        def x_take(masks, first, last):
            for t in range(first, last):
                for mask in masks:
                    src = sources[mask]
                    if t == 4:

                        @pl.when(src.x_count == SLOTS)
                        def _():
                            ex.take(mask, x_at(src, t), t)

                    else:
                        at = x_at(src, t)
                        ex.take(mask, at, t)
                        if (mask, t) in ((XN, 0), (XN + 2, 0), (YN, 1), (YN + 2, 1)):

                            @pl.when(at[2] == me)
                            def _():
                                buf[new, me, at[1]] = buf[new, at[1], at[2]].T

        def x_first(k, at, t):
            src = at[3]
            use_pair(new, at[1], (at[2], x_place(src, 1)[1]))

        def x_second(k, at, t):
            use_diag(new, at[1], at[2])

        def x_last(k, at, t):
            use(new, at[1], at[2])

        near = (PARTNER, XN, YN, XN + 2, YN + 2)
        far = (DIAG, DIAG + 2)
        ex.each((0,), x_first, 0, 1)
        ex.each((0,), x_second, 2, 3)
        ex.each((0,), x_last, 4, 5)
        x_take(near, 0, 2)
        ex.each(near, x_first, 0, 1)
        x_take(near, 2, 4)
        ex.each(near, x_second, 2, 3)
        x_take(near, 4, 5)
        ex.each(near, x_last, 4, 5)
        x_take(far, 0, 2)
        ex.each(far, x_first, 0, 1)
        x_take(far, 2, 4)
        ex.each(far, x_second, 2, 3)
        x_take(far, 4, 5)
        ex.each(far, x_last, 4, 5)
        before = ex

    old, end = (STEPS - 1) % 2, STEPS % 2
    before.drain()
    traces(old, STEPS)
    sums[2] = jnp.zeros((8, 128), jnp.float32)

    def other(q, mask):
        return 4 * flip(half(q, 4), half(mask, 4)) + 2 * flip(part(half(q)), part(half(mask))) + flip(part(q), part(mask))

    def last_copy(q, mask, to):
        block = buf.at[end, q, other(q, mask)]
        return pltpu.make_async_remote_copy(
            src_ref=block,
            dst_ref=block,
            send_sem=last_send.at[mask],
            recv_sem=last_recv.at[mask],
            device_id=device(to),
            device_id_type=MESH,
        )

    def put(row, b, val):
        out_ref[span(row - 4 * y), span(b)] = val

    def last_mask(d):
        return on * pick(d, (5, 4, 7, 6, 3, 0, 1, 2)) + (1 - on) * pick(d, (0, 2, 4, 5, 6, 7, 1, 3))

    def last_send_to(d):
        return on * pick(d, (4, 1, 6, 1, 2)) + (1 - on)

    def last_sends(d):
        return d < 2 + 3 * on

    @pl.loop(0, PANELS)
    def _(d):
        @pl.when(d < 6 + 2 * on)
        def _():
            mask = last_mask(d)
            col = other(me, mask)
            acc[...] = product(old, col)

            @pl.when(d == 0)
            def _():
                mix(STEPS)

            val = updated(old, col)

            @pl.when(last_sends(d))
            def _():
                buf[end, me, col] = val

            weight = 1 + on * part(mask) * (1 - half(mask, 4))
            sums[2] += fold(val * hrow[col]) * weight.astype(jnp.float32)

            @pl.when(last_sends(d))
            def _():
                last_copy(me, mask, last_send_to(d)).start()

            @pl.when(half(col, 4) == y)
            def _():
                put(col, y, val.T)

            @pl.when(jnp.logical_and(on == 1, mask == 1))
            def _():
                put(me, 1 - y, val)

    sum_start(STEPS + 1, [sums[2]])

    @pl.when(on == 1)
    def _():
        for mask, src in ((3, 2), (0, 1), (2, 1)):
            q = sources[src].q
            last_copy(q, jnp.int32(mask), jnp.int32(src)).wait_recv()
            col = other(q, jnp.int32(mask))
            if mask == 3:
                put(q, 1 - y, buf[end, q, col])
            else:
                put(col, 1 - y, buf[end, q, col].T)

    @pl.when(on == 0)
    def _():
        for mask, src in ((5, 4), (4, 1), (7, 6), (6, 1)):
            q = sources[src].q
            last_copy(q, jnp.int32(mask), jnp.int32(src)).wait_recv()
            col = other(q, jnp.int32(mask))
            if src == YN:
                put(col, 1 - y, buf[end, q, col].T)
            else:
                put(q, 1 - y, buf[end, q, col])

    @pl.loop(0, SLOTS)
    def _(d):
        @pl.when(last_sends(d))
        def _():
            last_copy(me, last_mask(d), last_send_to(d)).wait_send()

    (energy,) = sum_finish(STEPS + 1, 1)
    e_ref[0] = 2.0 * jnp.sum(energy)


def solution(mesh):
    n_cols = mesh.shape["col"]

    def local_fn(ham_blk, bounds, n_occ):
        rows_n, cols_n = ham_blk.shape
        n = cols_n * n_cols
        blk_n = n // PANELS
        f32 = jnp.float32
        return pl.pallas_call(
            lambda *refs: kernel(n, *refs),
            out_shape=(jax.ShapeDtypeStruct((rows_n, cols_n), f32), jax.ShapeDtypeStruct((1,), f32)),
            in_specs=[
                pl.BlockSpec(memory_space=pltpu.SMEM),
                pl.BlockSpec(memory_space=pltpu.SMEM),
                pl.BlockSpec(memory_space=pltpu.HBM),
            ],
            out_specs=(pl.BlockSpec(memory_space=pltpu.VMEM), pl.BlockSpec(memory_space=pltpu.SMEM)),
            scratch_shapes=[
                pltpu.VMEM((rows_n, cols_n), f32),
                pltpu.SemaphoreType.DMA,
                pltpu.VMEM((2, PANELS, PANELS, blk_n, blk_n), f32),
                pltpu.VMEM((PANELS, blk_n, blk_n), f32),
                pltpu.VMEM((PANELS, blk_n, blk_n), f32),
                pltpu.VMEM((blk_n, blk_n), f32),
                pltpu.VMEM((STEPS + 2, PANELS, 8, 128), f32),
                pltpu.VMEM((8, blk_n), f32),
                pltpu.VMEM((3, 8, 128), f32),
                pltpu.SemaphoreType.DMA((2, PANELS, SLOTS + CORNERS, 3)),
                pltpu.SemaphoreType.DMA((2, PANELS, SLOTS + CORNERS)),
                pltpu.SemaphoreType.DMA((STEPS + 2, PANELS)),
                pltpu.SemaphoreType.DMA((STEPS + 2, PANELS)),
                pltpu.SemaphoreType.DMA((PANELS,)),
                pltpu.SemaphoreType.DMA((PANELS,)),
            ],
            compiler_params=pltpu.CompilerParams(collective_id=0, has_side_effects=True, vmem_limit_bytes=48 << 20),
            name="purify",
        )(bounds, n_occ, ham_blk)

    spec_mat = P(("spin", "row"), "col")
    return jax.shard_map(local_fn, mesh=mesh, in_specs=(spec_mat, P("spin"), P("spin")), out_specs=(spec_mat, P("spin")), check_vma=False)
```

```python
import jax
import jax.numpy as jnp
from jax import lax
from jax.experimental import pallas as pl
from jax.experimental.pallas import tpu as pltpu
from jax.sharding import PartitionSpec as P

STEPS = 3
PANELS = 8
SLOTS = 5
CORNERS = 2
MESH = pl.DeviceIdType.MESH
NN = (((1,), (0,)), ((), ()))
NT = (((1,), (1,)), ((), ()))


def dot(lhs, rhs, dims):
    return lax.dot_general(lhs, rhs, dims, precision=lax.Precision.HIGHEST, preferred_element_type=jnp.float32)


def flag(cond):
    return lax.convert_element_type(cond, jnp.int32)


def pick(index, values):
    return sum(flag(index == k) * v for k, v in enumerate(values) if not (isinstance(v, int) and v == 0))


def half(val, by=2):
    return lax.div(val, jnp.int32(by))


def part(val, by=2):
    return lax.rem(val, jnp.int32(by))


def flip(bit, by):
    return bit + by - 2 * bit * by


def panel_bits(q):
    return q // 4, q % 2, (q // 2) % 2


def packed(digits, base):
    return sum(d * base**k for k, d in enumerate(digits))


def h_blocks(q):
    x, y, c = panel_bits(q)
    if x == y:
        local = {
            (0, 0): ((1, 0), (3, 0), (2, 0), (0, 0), (1, 1)),
            (0, 1): ((3, 0), (1, 0), (1, 1), (2, 0), (3, 1)),
            (1, 0): ((1, 0), (2, 0), (3, 0), (0, 0), (1, 1)),
            (1, 1): ((3, 0), (1, 0), (1, 1), (2, 0), (3, 1)),
        }[x, c]
    else:
        local = tuple((2 * k + (b + y) % 2, b) for b in range(2) for k in range(2))
    return tuple((4 * y + a, 4 * x + 2 * c + b) for a, b in local)


def x_blocks(q):
    x, y, c = panel_bits(q)
    return tuple(q ^ m for m in (4 + 2 * x, 1 + 2 * y, 5 + 2 * y, 0, 2, 7 - 2 * y))


def kernel(n, bounds, n_occ, h_hbm, out_ref, e_ref, h_ref, h_sem, buf, hrow, x2row, acc, parts, coef, sums, send_sem, recv_sem, part_send, part_recv, last_send, last_recv):
    blk_n = n // PANELS
    y = lax.axis_index("row")
    j = lax.axis_index("col")
    x, c = half(j), part(j)
    me = 4 * x + 2 * c + y
    on = 1 - flip(x, y)

    class Source:
        def __init__(self, q, h_pack, h_count, x_pack, x_count):
            self.fields = q, h_pack, h_count, x_pack, x_count
            self.q, self.h_pack, self.h_count, self.x_pack, self.x_count = self.fields

        def __add__(self, other):
            return Source(*(a + b for a, b in zip(self.fields, other.fields)))

        def __mul__(self, by):
            return Source(*(a * by for a in self.fields))

    def device(mask):
        dx, dy, dc = flip(x, half(mask, 4)), flip(y, part(mask)), flip(c, part(half(mask)))
        return (0, dy, 2 * dx + dc)

    def source(mask):
        q = panel(mask)
        return Source(
            q,
            pick(q, [packed([8 * row + col for row, col in h_blocks(k)], 64) for k in range(PANELS)]),
            pick(q, [len(h_blocks(k)) for k in range(PANELS)]),
            pick(q, [packed(x_blocks(k), 8) for k in range(PANELS)]),
            pick(q, [5 - (k // 2) % 2 for k in range(PANELS)]),
        )

    def panel(mask):
        return 4 * flip(x, mask // 4) + 2 * flip(c, (mask // 2) % 2) + flip(y, mask % 2)

    def h_place(src, t):
        code = part(lax.div(src.h_pack, pick(t, [64**k for k in range(SLOTS)])), 64)
        return half(code, 8), part(code, 8)

    def x_place(src, t):
        return src.q, part(lax.div(src.x_pack, pick(t, [8**k for k in range(SLOTS + 1)])), 8)

    def x_at(src, t):
        return src.q, src.q, part(half(src.x_pack, 8**t), 8), src

    devices = [device(jnp.int32(mask)) for mask in range(8)]
    sources = [source(mask) for mask in range(8)]

    PARTNER, XN, YN, DIAG = 2, 4, 1, 5

    h_in = pltpu.make_async_copy(h_hbm, h_ref, h_sem)
    h_in.start()

    barrier = pltpu.get_barrier_semaphore()
    for mask in range(1, 8):
        pl.semaphore_signal(barrier, inc=1, device_id=devices[mask], device_id_type=MESH)
    pl.semaphore_wait(barrier, 7)
    h_in.wait()

    class Exchange:
        def __init__(self, rnd, buf_id, place, count, own_src=None):
            self.rnd, self.buf_id, self.place, self.count = rnd, buf_id, place, count
            self.own_src = own_src or (lambda row, col: buf.at[buf_id, row, col])

        def copy(self, at, t, way, view, src=None):
            q, row, col, _ = at
            block = view(buf.at[self.buf_id, row, col])
            return pltpu.make_async_remote_copy(
                src_ref=block if src is None else view(src),
                dst_ref=block,
                send_sem=send_sem.at[self.rnd, q, t, way],
                recv_sem=recv_sem.at[self.rnd, q, t],
                device_id=devices[(PARTNER, XN, YN)[way]],
                device_id_type=MESH,
            )

        def pieces(self, at, t, body):
            mid = blk_n // 2

            @pl.when(at[1] != at[2])
            def _():
                body(t, lambda ref: ref, flag(t == 0) + flag(t == 2))

            @pl.when(at[1] == at[2])
            def _():
                body(t, lambda ref: ref.at[pl.ds(0, mid), :], jnp.int32(0))
                body(t + CORNERS, lambda ref: ref.at[pl.ds(mid, mid), pl.ds(mid, mid)], flag(t == 4))

        def own(self, at, t, act):
            def body(slot, view, x_way):
                for way in range(3):
                    act(self.copy(at, slot, way, view, self.own_src(*at[1:3])))

            self.pieces(at, t, body)

        def forward(self, mask, at, t, act):
            def body(slot, view, x_way):
                act(self.copy(at, slot, 0, view))
                if mask == XN:

                    @pl.when(x_way == 1)
                    def _():
                        act(self.copy(at, slot, 2, view))

                if mask == YN:

                    @pl.when(x_way == 0)
                    def _():
                        act(self.copy(at, slot, 1, view))

            self.pieces(at, t, body)

        def forward_any(self, k, masks, at, t, act):
            for mask in (XN, YN, DIAG):
                if mask in masks:

                    @pl.when(k == masks.index(mask))
                    def _():
                        self.forward(mask, at, t, act)

        def arrive(self, k, masks, at, t):
            self.pieces(at, t, lambda slot, view, x_way: self.copy(at, slot, 0, view).wait_recv())
            self.forward_any(k, masks, at, t, lambda copy: copy.start())
            mid = blk_n // 2

            @pl.when(at[1] == at[2])
            def _():
                block = buf.at[self.buf_id, at[1], at[2]]
                block[mid:, :mid] = block[:mid, mid:].T

        def take(self, mask, at, t):
            mid = blk_n // 2
            views = [(t, lambda ref: ref)]
            if t == 3:
                views = [(t, lambda ref: ref.at[pl.ds(0, mid), :]), (t + CORNERS, lambda ref: ref.at[pl.ds(mid, mid), pl.ds(mid, mid)])]
            for slot, view in views:
                self.copy(at, slot, 0, view).wait_recv()
            for slot, view in views:
                if mask in (XN, YN, DIAG):
                    self.copy(at, slot, 0, view).start()
                if mask == XN and t in (0, 2):
                    self.copy(at, slot, 2, view).start()
                if mask == YN and t not in (0, 2):
                    self.copy(at, slot, 1, view).start()
            if t == 3:
                block = buf.at[self.buf_id, at[1], at[2]]
                block[mid:, :mid] = block[:mid, mid:].T

        def at(self, src, t):
            return (src.q, *self.place(src, t), src)

        def each(self, masks, body, first=0, last=SLOTS):
            srcs = [mask if isinstance(mask, Source) else sources[mask] for mask in masks]
            many = len(srcs)

            @pl.loop(0, (last - first) * many)
            def _(i):
                t, k = first + half(i, many), part(i, many)
                src = srcs[0] if many == 1 else Source(*(pick(k, vals) for vals in zip(*(src.fields for src in srcs))))

                @pl.when(t < self.count(src))
                def _():
                    body(k, self.at(src, t), t)

        def drain(self):
            self.each((0,), lambda k, at, t: self.own(at, t, lambda copy: copy.wait_send()))
            far = (XN, YN, DIAG)
            self.each(far, lambda k, at, t: self.forward_any(k, far, at, t, lambda copy: copy.wait_send()))

    def part_copy(rnd, src, mask):
        return pltpu.make_async_remote_copy(
            src_ref=parts.at[rnd, src],
            dst_ref=parts.at[rnd, src],
            send_sem=part_send.at[rnd, mask],
            recv_sem=part_recv.at[rnd, src],
            device_id=devices[mask],
            device_id_type=MESH,
        )

    def sum_start(rnd, vals):
        for k, val in enumerate(vals):
            parts[rnd, me, k : k + 1] = jnp.sum(val, axis=0, keepdims=True)
        for mask in range(1, 8):
            part_copy(rnd, me, mask).start()

    def sum_finish(rnd, count):
        for mask in range(1, 8):
            part_copy(rnd, sources[mask].q, mask).wait_recv()
        for mask in range(1, 8):
            part_copy(rnd, me, mask).wait_send()
        tot = parts[rnd, 0]
        for q in range(1, PANELS):
            tot = tot + parts[rnd, q]
        return [jnp.sum(tot[k : k + 1], axis=1, keepdims=True) for k in range(count)]

    def fold(val):
        rows, cols = val.shape
        val = jnp.sum(val.reshape(rows // 8, 8, cols), axis=0)
        tot = val[:, :128]
        for k in range(1, cols // 128):
            tot = tot + val[:, k * 128 : (k + 1) * 128]
        return tot

    def span(k):
        return pl.ds(pl.multiple_of(k * blk_n, blk_n), blk_n)

    def clear():
        @pl.loop(0, PANELS)
        def _(col):
            x2row[col] = jnp.zeros((blk_n, blk_n), jnp.float32)

    def h_src(row, col):
        return h_ref.at[span(row - 4 * y), span(col - 2 * j)]

    hx = Exchange(0, 1, h_place, lambda src: src.h_count, h_src)
    hx.each((0,), lambda k, at, t: hx.own(at, t, lambda copy: copy.start()))

    rows_n, cols_n = h_ref.shape
    mu_part = jnp.zeros((8, 128), jnp.float32)
    for k in range(rows_n // blk_n):
        tile = h_ref[k * blk_n : (k + 1) * blk_n, :]
        row_ids = y * rows_n + k * blk_n + lax.broadcasted_iota(jnp.int32, tile.shape, 0)
        col_ids = j * cols_n + lax.broadcasted_iota(jnp.int32, tile.shape, 1)
        mu_part = mu_part + fold(jnp.where(row_ids == col_ids, tile, 0.0))
    sum_start(0, [mu_part])
    clear()

    eye = (lax.broadcasted_iota(jnp.int32, (blk_n, blk_n), 0) == lax.broadcasted_iota(jnp.int32, (blk_n, blk_n), 1)).astype(jnp.float32)
    (trace_h,) = sum_finish(0, 1)
    occ = n_occ[0].astype(jnp.float32)
    mu = trace_h / n
    lam = jnp.minimum(occ / (bounds[1] - mu), (n - occ) / (mu - bounds[0]))
    coef[0:1, :] = jnp.broadcast_to(lam / n, (1, blk_n))
    coef[1:2, :] = jnp.broadcast_to(mu, (1, blk_n))
    coef[2:3, :] = jnp.broadcast_to(jnp.full((1, 1), occ / n, jnp.float32), (1, blk_n))

    def first_x(own, at):
        _, row, col = at[:3]
        blk = h_src(row, col)[...] if own else buf[1, row, col]
        diag = eye * (row == col).astype(jnp.float32)
        val = coef[0:1, :] * (coef[1:2, :] * diag - blk) + coef[2:3, :] * diag
        buf[0, row, col] = val

        @pl.when(row != col)
        def _():
            buf[0, col, row] = val.T

        @pl.when(row == me)
        def _():
            hrow[col] = blk

        @pl.when(jnp.logical_and(col == me, row != me))
        def _():
            hrow[row] = blk.T

    def use(b, row, col):
        blk = buf[b, row, col]
        x2row[col] += dot(buf[b, me, row], blk, NN)
        x2row[row] += dot(buf[b, me, col], blk, NT)
        buf[b, col, row] = blk.T

    def use_pair(b, row, col):
        blk = [buf[b, row, k] for k in col]
        left = buf[b, me, row]
        right = [buf[b, me, k] for k in col]
        for k in range(2):
            x2row[col[k]] += dot(left, blk[k], NN)
        x2row[row] += dot(right[0], blk[0], NT) + dot(right[1], blk[1], NT)
        for k in range(2):
            buf[b, col[k], row] = blk[k].T

    def use_diag(b, row, col):
        blk, mid = buf[b, row, col], buf[b, row, row]
        left = buf[b, me, row]
        right = buf[b, me, col]
        x2row[col] += dot(left, blk, NN)
        x2row[row] += dot(right, blk, NT) + dot(left, mid, NN)
        buf[b, col, row] = blk.T

    def h_take(masks):
        def body(k, at, t):
            hx.arrive(k, masks, at, t)
            first_x(False, at)

        return body

    def h_unit(col, kind):
        cross = half(kind)
        first = 4 * flip(half(col, 4), cross) + (1 - cross) * 2 * kind + cross * flip(part(col), part(kind))
        second = first + 1 + cross
        x2row[col] += dot(buf[0, me, first], buf[0, first, col], NN) + dot(buf[0, me, second], buf[0, second, col], NN)

    @pl.loop(0, 4)
    def _(k):
        first_x(True, (me, 4 * y + k, me))

    hx.each((0,), lambda k, at, t: first_x(True, at))
    hx.each((PARTNER,), h_take((PARTNER,)))

    near = (XN, YN, XN + 2, YN + 2)
    far = (DIAG, DIAG + 2)
    off = 1 - on
    hx.each(near, h_take(near), 0, 1)

    @pl.loop(0, 4 + 4 * on)
    def _(i):
        h_unit(on * (4 * y + half(i)) + off * (4 - 4 * y + i), on * part(i) + off * (2 + y))

    hx.each(near, h_take(near), 1, 3)

    @pl.loop(0, 4 * off)
    def _(i):
        h_unit(4 * y + i, 1 - half(i))

    hx.each(near, h_take(near), 3, SLOTS)

    @pl.loop(0, 16)
    def _(i):
        col, kind = on * (4 * flip(y, half(i, 8)) + half(part(i, 8))) + off * half(i), on * 2 + part(i)

        @pl.when(on + flag(half(col, 4) != y) + flag(kind == half(part(col, 4))) > 0)
        def _():
            h_unit(col, kind)

    @pl.loop(0, 4 * off)
    def _(i):
        h_unit(4 * y + i, 2 + y)

    hx.each(far, h_take(far), 0, 2)

    @pl.loop(0, 4 * off)
    def _(i):
        late_half = half(i)
        h_unit(4 * flip(y, late_half) + 2 * part(i) + late_half * (1 - y), 3 - y)

    hx.each(far, h_take(far), 2, SLOTS)

    @pl.loop(0, 4 + 4 * on)
    def _(i):
        late_half = half(i)
        h_unit(on * (4 - 4 * y + half(i)) + off * (4 * flip(y, late_half) + 2 * part(i) + 1 - late_half * (1 - y)), on * part(i) + off * (3 - y))

    def product(old, col):
        tot = dot(x2row[0], buf[old, 0, col], NN)
        for k in range(1, PANELS):
            tot = tot + dot(x2row[k], buf[old, k, col], NN)
        return tot

    def traces(old, rnd):
        t1 = fold(buf[old, me, me] * eye)
        sums[...] = jnp.zeros_like(sums)

        @pl.loop(0, PANELS)
        def _(col):
            xv = buf[old, me, col]
            sums[0] += fold(xv * xv)
            sums[1] += fold(xv * x2row[col])

        sum_start(rnd, [t1, sums[0], sums[1]])

    def mix(rnd):
        t1, t2, t3 = sum_finish(rnd, 3)
        cval = (t2 - t3) / (t1 - t2)
        inv = 1.0 / (1.0 - cval)
        for k, val in enumerate(((1.0 - 2.0 * cval) * inv, (1.0 + cval) * inv, inv)):
            coef[k : k + 1, :] = jnp.broadcast_to(val, (1, blk_n))

    def updated(old, col):
        return coef[0:1, :] * buf[old, me, col] + coef[1:2, :] * x2row[col] - coef[2:3, :] * acc[...]

    hx.drain()

    @pl.loop(0, STEPS - 1)
    def _(step):
        old, new = part(step), part(step + 1)
        traces(old, 1 + step)
        ex = Exchange(part(1 + step), new, x_place, lambda src: src.x_count)

        @pl.loop(0, SLOTS + 1)
        def _(t):
            at = ex.at(sources[0], t)
            col = at[2]
            acc[...] = product(old, col)

            @pl.when(t == 0)
            def _():
                mix(1 + step)

            buf[new, me, col] = updated(old, col)

            @pl.when(t < sources[0].x_count)
            def _():
                ex.own(at, t, lambda copy: copy.start())

        clear()

        def x_take(masks, first, last):
            for t in range(first, last):
                for mask in masks:
                    src = sources[mask]
                    if t == 4:

                        @pl.when(src.x_count == SLOTS)
                        def _():
                            ex.take(mask, x_at(src, t), t)

                    else:
                        at = x_at(src, t)
                        ex.take(mask, at, t)
                        if (mask, t) in ((XN, 0), (XN + 2, 0), (YN, 1), (YN + 2, 1)):

                            @pl.when(at[2] == me)
                            def _():
                                buf[new, me, at[1]] = buf[new, at[1], at[2]].T

        def x_first(k, at, t):
            src = at[3]
            use_pair(new, at[1], (at[2], x_place(src, 1)[1]))

        def x_second(k, at, t):
            use_diag(new, at[1], at[2])

        def x_last(k, at, t):
            use(new, at[1], at[2])

        near = (PARTNER, XN, YN, XN + 2, YN + 2)
        far = (DIAG, DIAG + 2)
        ex.each((0,), x_first, 0, 1)
        ex.each((0,), x_second, 2, 3)
        ex.each((0,), x_last, 4, 5)
        x_take(near, 0, 2)
        ex.each(near, x_first, 0, 1)
        x_take(near, 2, 4)
        ex.each(near, x_second, 2, 3)
        x_take(near, 4, 5)
        ex.each(near, x_last, 4, 5)
        x_take(far, 0, 2)
        ex.each(far, x_first, 0, 1)
        x_take(far, 2, 4)
        ex.each(far, x_second, 2, 3)
        x_take(far, 4, 5)
        ex.each(far, x_last, 4, 5)
        ex.drain()

    old, end = (STEPS - 1) % 2, STEPS % 2
    traces(old, STEPS)
    sums[2] = jnp.zeros((8, 128), jnp.float32)

    def other(q, mask):
        return 4 * flip(half(q, 4), half(mask, 4)) + 2 * flip(part(half(q)), part(half(mask))) + flip(part(q), part(mask))

    def last_copy(q, mask, to):
        block = buf.at[end, q, other(q, mask)]
        return pltpu.make_async_remote_copy(
            src_ref=block,
            dst_ref=block,
            send_sem=last_send.at[mask],
            recv_sem=last_recv.at[mask],
            device_id=device(to),
            device_id_type=MESH,
        )

    def put(row, b, val):
        out_ref[span(row - 4 * y), span(b)] = val

    def last_mask(d):
        return on * pick(d, (5, 4, 7, 6, 3, 0, 1, 2)) + (1 - on) * pick(d, (0, 2, 4, 5, 6, 7, 1, 3))

    def last_send_to(d):
        return on * pick(d, (4, 1, 6, 1, 2)) + (1 - on)

    def last_sends(d):
        return d < 2 + 3 * on

    @pl.loop(0, PANELS)
    def _(d):
        @pl.when(d < 6 + 2 * on)
        def _():
            mask = last_mask(d)
            col = other(me, mask)
            acc[...] = product(old, col)

            @pl.when(d == 0)
            def _():
                mix(STEPS)

            val = updated(old, col)

            @pl.when(last_sends(d))
            def _():
                buf[end, me, col] = val

            weight = 1 + on * part(mask) * (1 - half(mask, 4))
            sums[2] += fold(val * hrow[col]) * weight.astype(jnp.float32)

            @pl.when(last_sends(d))
            def _():
                last_copy(me, mask, last_send_to(d)).start()

            @pl.when(half(col, 4) == y)
            def _():
                put(col, y, val.T)

            @pl.when(jnp.logical_and(on == 1, mask == 1))
            def _():
                put(me, 1 - y, val)

    sum_start(STEPS + 1, [sums[2]])

    @pl.when(on == 1)
    def _():
        for mask, src in ((3, 2), (0, 1), (2, 1)):
            q = sources[src].q
            last_copy(q, jnp.int32(mask), jnp.int32(src)).wait_recv()
            col = other(q, jnp.int32(mask))
            if mask == 3:
                put(q, 1 - y, buf[end, q, col])
            else:
                put(col, 1 - y, buf[end, q, col].T)

    @pl.when(on == 0)
    def _():
        for mask, src in ((5, 4), (4, 1), (7, 6), (6, 1)):
            q = sources[src].q
            last_copy(q, jnp.int32(mask), jnp.int32(src)).wait_recv()
            col = other(q, jnp.int32(mask))
            if src == YN:
                put(col, 1 - y, buf[end, q, col].T)
            else:
                put(q, 1 - y, buf[end, q, col])

    @pl.loop(0, SLOTS)
    def _(d):
        @pl.when(last_sends(d))
        def _():
            last_copy(me, last_mask(d), last_send_to(d)).wait_send()

    (energy,) = sum_finish(STEPS + 1, 1)
    e_ref[0] = 2.0 * jnp.sum(energy)


def solution(mesh):
    n_cols = mesh.shape["col"]

    def local_fn(ham_blk, bounds, n_occ):
        rows_n, cols_n = ham_blk.shape
        n = cols_n * n_cols
        blk_n = n // PANELS
        f32 = jnp.float32
        return pl.pallas_call(
            lambda *refs: kernel(n, *refs),
            out_shape=(jax.ShapeDtypeStruct((rows_n, cols_n), f32), jax.ShapeDtypeStruct((1,), f32)),
            in_specs=[
                pl.BlockSpec(memory_space=pltpu.SMEM),
                pl.BlockSpec(memory_space=pltpu.SMEM),
                pl.BlockSpec(memory_space=pltpu.HBM),
            ],
            out_specs=(pl.BlockSpec(memory_space=pltpu.VMEM), pl.BlockSpec(memory_space=pltpu.SMEM)),
            scratch_shapes=[
                pltpu.VMEM((rows_n, cols_n), f32),
                pltpu.SemaphoreType.DMA,
                pltpu.VMEM((2, PANELS, PANELS, blk_n, blk_n), f32),
                pltpu.VMEM((PANELS, blk_n, blk_n), f32),
                pltpu.VMEM((PANELS, blk_n, blk_n), f32),
                pltpu.VMEM((blk_n, blk_n), f32),
                pltpu.VMEM((STEPS + 2, PANELS, 8, 128), f32),
                pltpu.VMEM((8, blk_n), f32),
                pltpu.VMEM((3, 8, 128), f32),
                pltpu.SemaphoreType.DMA((2, PANELS, SLOTS + CORNERS, 3)),
                pltpu.SemaphoreType.DMA((2, PANELS, SLOTS + CORNERS)),
                pltpu.SemaphoreType.DMA((STEPS + 2, PANELS)),
                pltpu.SemaphoreType.DMA((STEPS + 2, PANELS)),
                pltpu.SemaphoreType.DMA((PANELS,)),
                pltpu.SemaphoreType.DMA((PANELS,)),
            ],
            compiler_params=pltpu.CompilerParams(collective_id=0, has_side_effects=True, vmem_limit_bytes=48 << 20),
            name="purify",
        )(bounds, n_occ, ham_blk)

    spec_mat = P(("spin", "row"), "col")
    return jax.shard_map(local_fn, mesh=mesh, in_specs=(spec_mat, P("spin"), P("spin")), out_specs=(spec_mat, P("spin")), check_vma=False)
```

```python
import jax
import jax.numpy as jnp
from jax import lax
from jax.experimental import pallas as pl
from jax.experimental.pallas import tpu as pltpu
from jax.sharding import PartitionSpec as P

STEPS = 3
PANELS = 8
SLOTS = 5
CORNERS = 2
MESH = pl.DeviceIdType.MESH
NN = (((1,), (0,)), ((), ()))
NT = (((1,), (1,)), ((), ()))


def dot(lhs, rhs, dims):
    return lax.dot_general(lhs, rhs, dims, precision=lax.Precision.HIGHEST, preferred_element_type=jnp.float32)


def flag(cond):
    return lax.convert_element_type(cond, jnp.int32)


def pick(index, values):
    return sum(flag(index == k) * v for k, v in enumerate(values) if not (isinstance(v, int) and v == 0))


def half(val, by=2):
    return lax.div(val, jnp.int32(by))


def part(val, by=2):
    return lax.rem(val, jnp.int32(by))


def flip(bit, by):
    return bit + by - 2 * bit * by


def panel_bits(q):
    return q // 4, q % 2, (q // 2) % 2


def packed(digits, base):
    return sum(d * base**k for k, d in enumerate(digits))


def h_blocks(q):
    x, y, c = panel_bits(q)
    if x == y:
        local = {
            (0, 0): ((1, 0), (3, 0), (2, 0), (0, 0), (1, 1)),
            (0, 1): ((3, 0), (1, 0), (1, 1), (2, 0), (3, 1)),
            (1, 0): ((1, 0), (2, 0), (3, 0), (0, 0), (1, 1)),
            (1, 1): ((3, 0), (1, 0), (1, 1), (2, 0), (3, 1)),
        }[x, c]
    else:
        local = tuple((2 * k + (b + y) % 2, b) for b in range(2) for k in range(2))
    return tuple((4 * y + a, 4 * x + 2 * c + b) for a, b in local)


def x_blocks(q):
    x, y, c = panel_bits(q)
    return tuple(q ^ m for m in (4 + 2 * x, 1 + 2 * y, 5 + 2 * y, 0, 2, 7 - 2 * y))


def kernel(n, bounds, n_occ, h_hbm, out_ref, e_ref, h_ref, h_sem, buf, hrow, x2row, acc, parts, coef, sums, send_sem, recv_sem, part_send, part_recv, last_send, last_recv):
    blk_n = n // PANELS
    y = lax.axis_index("row")
    j = lax.axis_index("col")
    x, c = half(j), part(j)
    me = 4 * x + 2 * c + y
    on = 1 - flip(x, y)

    class Source:
        def __init__(self, q, h_pack, h_count, x_pack, x_count):
            self.fields = q, h_pack, h_count, x_pack, x_count
            self.q, self.h_pack, self.h_count, self.x_pack, self.x_count = self.fields

        def __add__(self, other):
            return Source(*(a + b for a, b in zip(self.fields, other.fields)))

        def __mul__(self, by):
            return Source(*(a * by for a in self.fields))

    def device(mask):
        dx, dy, dc = flip(x, half(mask, 4)), flip(y, part(mask)), flip(c, part(half(mask)))
        return (0, dy, 2 * dx + dc)

    def source(mask):
        q = panel(mask)
        return Source(
            q,
            pick(q, [packed([8 * row + col for row, col in h_blocks(k)], 64) for k in range(PANELS)]),
            pick(q, [len(h_blocks(k)) for k in range(PANELS)]),
            pick(q, [packed(x_blocks(k), 8) for k in range(PANELS)]),
            pick(q, [5 - (k // 2) % 2 for k in range(PANELS)]),
        )

    def panel(mask):
        return 4 * flip(x, mask // 4) + 2 * flip(c, (mask // 2) % 2) + flip(y, mask % 2)

    def h_place(src, t):
        code = part(lax.div(src.h_pack, pick(t, [64**k for k in range(SLOTS)])), 64)
        return half(code, 8), part(code, 8)

    def x_place(src, t):
        return src.q, part(lax.div(src.x_pack, pick(t, [8**k for k in range(SLOTS + 1)])), 8)

    def x_at(src, t):
        return src.q, src.q, part(half(src.x_pack, 8**t), 8), src

    devices = [device(jnp.int32(mask)) for mask in range(8)]
    sources = [source(mask) for mask in range(8)]

    PARTNER, XN, YN, DIAG = 2, 4, 1, 5

    h_in = pltpu.make_async_copy(h_hbm, h_ref, h_sem)
    h_in.start()

    barrier = pltpu.get_barrier_semaphore()
    for mask in range(1, 8):
        pl.semaphore_signal(barrier, inc=1, device_id=devices[mask], device_id_type=MESH)
    pl.semaphore_wait(barrier, 7)
    h_in.wait()

    class Exchange:
        def __init__(self, buf_id, place, count, own_src=None):
            self.buf_id, self.place, self.count = buf_id, place, count
            self.own_src = own_src or (lambda row, col: buf.at[buf_id, row, col])

        def copy(self, at, t, way, view, src=None):
            q, row, col, _ = at
            block = view(buf.at[self.buf_id, row, col])
            return pltpu.make_async_remote_copy(
                src_ref=block if src is None else view(src),
                dst_ref=block,
                send_sem=send_sem.at[q, t, way],
                recv_sem=recv_sem.at[q, t],
                device_id=devices[(PARTNER, XN, YN)[way]],
                device_id_type=MESH,
            )

        def pieces(self, at, t, body):
            mid = blk_n // 2

            @pl.when(at[1] != at[2])
            def _():
                body(t, lambda ref: ref, flag(t == 0) + flag(t == 2))

            @pl.when(at[1] == at[2])
            def _():
                body(t, lambda ref: ref.at[pl.ds(0, mid), :], jnp.int32(0))
                body(t + CORNERS, lambda ref: ref.at[pl.ds(mid, mid), pl.ds(mid, mid)], flag(t == 4))

        def own(self, at, t, act):
            def body(slot, view, x_way):
                for way in range(3):
                    act(self.copy(at, slot, way, view, self.own_src(*at[1:3])))

            self.pieces(at, t, body)

        def forward(self, mask, at, t, act):
            def body(slot, view, x_way):
                act(self.copy(at, slot, 0, view))
                if mask == XN:

                    @pl.when(x_way == 1)
                    def _():
                        act(self.copy(at, slot, 2, view))

                if mask == YN:

                    @pl.when(x_way == 0)
                    def _():
                        act(self.copy(at, slot, 1, view))

            self.pieces(at, t, body)

        def forward_any(self, k, masks, at, t, act):
            for mask in (XN, YN, DIAG):
                if mask in masks:

                    @pl.when(k == masks.index(mask))
                    def _():
                        self.forward(mask, at, t, act)

        def arrive(self, k, masks, at, t):
            self.pieces(at, t, lambda slot, view, x_way: self.copy(at, slot, 0, view).wait_recv())
            self.forward_any(k, masks, at, t, lambda copy: copy.start())
            mid = blk_n // 2

            @pl.when(at[1] == at[2])
            def _():
                block = buf.at[self.buf_id, at[1], at[2]]
                block[mid:, :mid] = block[:mid, mid:].T

        def take(self, mask, at, t):
            mid = blk_n // 2
            views = [(t, lambda ref: ref)]
            if t == 3:
                views = [(t, lambda ref: ref.at[pl.ds(0, mid), :]), (t + CORNERS, lambda ref: ref.at[pl.ds(mid, mid), pl.ds(mid, mid)])]
            for slot, view in views:
                self.copy(at, slot, 0, view).wait_recv()
            for slot, view in views:
                if mask in (XN, YN, DIAG):
                    self.copy(at, slot, 0, view).start()
                if mask == XN and t in (0, 2):
                    self.copy(at, slot, 2, view).start()
                if mask == YN and t not in (0, 2):
                    self.copy(at, slot, 1, view).start()
            if t == 3:
                block = buf.at[self.buf_id, at[1], at[2]]
                block[mid:, :mid] = block[:mid, mid:].T

        def at(self, src, t):
            return (src.q, *self.place(src, t), src)

        def each(self, masks, body, first=0, last=SLOTS):
            srcs = [mask if isinstance(mask, Source) else sources[mask] for mask in masks]
            many = len(srcs)

            @pl.loop(0, (last - first) * many)
            def _(i):
                t, k = first + half(i, many), part(i, many)
                src = srcs[0] if many == 1 else Source(*(pick(k, vals) for vals in zip(*(src.fields for src in srcs))))

                @pl.when(t < self.count(src))
                def _():
                    body(k, self.at(src, t), t)

        def drain(self):
            self.each((0,), lambda k, at, t: self.own(at, t, lambda copy: copy.wait_send()))
            far = (XN, YN, DIAG)
            self.each(far, lambda k, at, t: self.forward_any(k, far, at, t, lambda copy: copy.wait_send()))

    def part_copy(rnd, src, mask):
        return pltpu.make_async_remote_copy(
            src_ref=parts.at[rnd, src],
            dst_ref=parts.at[rnd, src],
            send_sem=part_send.at[mask],
            recv_sem=part_recv.at[rnd, src],
            device_id=devices[mask],
            device_id_type=MESH,
        )

    def sum_start(rnd, vals):
        for k, val in enumerate(vals):
            parts[rnd, me, k : k + 1] = jnp.sum(val, axis=0, keepdims=True)
        for mask in range(1, 8):
            part_copy(rnd, me, mask).start()

    def sum_finish(rnd, count):
        for mask in range(1, 8):
            part_copy(rnd, sources[mask].q, mask).wait_recv()
        for mask in range(1, 8):
            part_copy(rnd, me, mask).wait_send()
        tot = parts[rnd, 0]
        for q in range(1, PANELS):
            tot = tot + parts[rnd, q]
        return [jnp.sum(tot[k : k + 1], axis=1, keepdims=True) for k in range(count)]

    def fold(val):
        rows, cols = val.shape
        val = jnp.sum(val.reshape(rows // 8, 8, cols), axis=0)
        tot = val[:, :128]
        for k in range(1, cols // 128):
            tot = tot + val[:, k * 128 : (k + 1) * 128]
        return tot

    def span(k):
        return pl.ds(pl.multiple_of(k * blk_n, blk_n), blk_n)

    def clear():
        @pl.loop(0, PANELS)
        def _(col):
            x2row[col] = jnp.zeros((blk_n, blk_n), jnp.float32)

    def h_src(row, col):
        return h_ref.at[span(row - 4 * y), span(col - 2 * j)]

    hx = Exchange(1, h_place, lambda src: src.h_count, h_src)
    hx.each((0,), lambda k, at, t: hx.own(at, t, lambda copy: copy.start()))

    rows_n, cols_n = h_ref.shape
    mu_part = jnp.zeros((8, 128), jnp.float32)
    for k in range(rows_n // blk_n):
        tile = h_ref[k * blk_n : (k + 1) * blk_n, :]
        row_ids = y * rows_n + k * blk_n + lax.broadcasted_iota(jnp.int32, tile.shape, 0)
        col_ids = j * cols_n + lax.broadcasted_iota(jnp.int32, tile.shape, 1)
        mu_part = mu_part + fold(jnp.where(row_ids == col_ids, tile, 0.0))
    sum_start(0, [mu_part])
    clear()

    eye = (lax.broadcasted_iota(jnp.int32, (blk_n, blk_n), 0) == lax.broadcasted_iota(jnp.int32, (blk_n, blk_n), 1)).astype(jnp.float32)
    (trace_h,) = sum_finish(0, 1)
    occ = n_occ[0].astype(jnp.float32)
    mu = trace_h / n
    lam = jnp.minimum(occ / (bounds[1] - mu), (n - occ) / (mu - bounds[0]))
    coef[0:1, :] = jnp.broadcast_to(lam / n, (1, blk_n))
    coef[1:2, :] = jnp.broadcast_to(mu, (1, blk_n))
    coef[2:3, :] = jnp.broadcast_to(jnp.full((1, 1), occ / n, jnp.float32), (1, blk_n))

    def first_x(own, at):
        _, row, col = at[:3]
        blk = h_src(row, col)[...] if own else buf[1, row, col]
        diag = eye * (row == col).astype(jnp.float32)
        val = coef[0:1, :] * (coef[1:2, :] * diag - blk) + coef[2:3, :] * diag
        buf[0, row, col] = val

        @pl.when(row != col)
        def _():
            buf[0, col, row] = val.T

        @pl.when(row == me)
        def _():
            hrow[col] = blk

        @pl.when(jnp.logical_and(col == me, row != me))
        def _():
            hrow[row] = blk.T

    def use(b, row, col):
        blk = buf[b, row, col]
        x2row[col] += dot(buf[b, me, row], blk, NN)
        x2row[row] += dot(buf[b, me, col], blk, NT)
        buf[b, col, row] = blk.T

    def use_pair(b, row, col):
        blk = [buf[b, row, k] for k in col]
        left = buf[b, me, row]
        right = [buf[b, me, k] for k in col]
        for k in range(2):
            x2row[col[k]] += dot(left, blk[k], NN)
        x2row[row] += dot(right[0], blk[0], NT) + dot(right[1], blk[1], NT)
        for k in range(2):
            buf[b, col[k], row] = blk[k].T

    def use_diag(b, row, col):
        blk, mid = buf[b, row, col], buf[b, row, row]
        left = buf[b, me, row]
        right = buf[b, me, col]
        x2row[col] += dot(left, blk, NN)
        x2row[row] += dot(right, blk, NT) + dot(left, mid, NN)
        buf[b, col, row] = blk.T

    def h_take(masks):
        def body(k, at, t):
            hx.arrive(k, masks, at, t)
            first_x(False, at)

        return body

    def h_unit(col, kind):
        cross = half(kind)
        first = 4 * flip(half(col, 4), cross) + (1 - cross) * 2 * kind + cross * flip(part(col), part(kind))
        second = first + 1 + cross
        x2row[col] += dot(buf[0, me, first], buf[0, first, col], NN) + dot(buf[0, me, second], buf[0, second, col], NN)

    @pl.loop(0, 4)
    def _(k):
        first_x(True, (me, 4 * y + k, me))

    hx.each((0,), lambda k, at, t: first_x(True, at))
    hx.each((PARTNER,), h_take((PARTNER,)))

    near = (XN, YN, XN + 2, YN + 2)
    far = (DIAG, DIAG + 2)
    off = 1 - on
    hx.each(near, h_take(near), 0, 1)

    @pl.loop(0, 4 + 4 * on)
    def _(i):
        h_unit(on * (4 * y + half(i)) + off * (4 - 4 * y + i), on * part(i) + off * (2 + y))

    hx.each(near, h_take(near), 1, 3)

    @pl.loop(0, 4 * off)
    def _(i):
        h_unit(4 * y + i, 1 - half(i))

    hx.each(near, h_take(near), 3, SLOTS)

    @pl.loop(0, 16)
    def _(i):
        col, kind = on * (4 * flip(y, half(i, 8)) + half(part(i, 8))) + off * half(i), on * 2 + part(i)

        @pl.when(on + flag(half(col, 4) != y) + flag(kind == half(part(col, 4))) > 0)
        def _():
            h_unit(col, kind)

    @pl.loop(0, 4 * off)
    def _(i):
        h_unit(4 * y + i, 2 + y)

    hx.each(far, h_take(far), 0, 2)

    @pl.loop(0, 4 * off)
    def _(i):
        late_half = half(i)
        h_unit(4 * flip(y, late_half) + 2 * part(i) + late_half * (1 - y), 3 - y)

    hx.each(far, h_take(far), 2, SLOTS)

    @pl.loop(0, 4 + 4 * on)
    def _(i):
        late_half = half(i)
        h_unit(on * (4 - 4 * y + half(i)) + off * (4 * flip(y, late_half) + 2 * part(i) + 1 - late_half * (1 - y)), on * part(i) + off * (3 - y))

    def product(old, col):
        tot = dot(x2row[0], buf[old, 0, col], NN)
        for k in range(1, PANELS):
            tot = tot + dot(x2row[k], buf[old, k, col], NN)
        return tot

    def traces(old, rnd):
        t1 = fold(buf[old, me, me] * eye)
        sums[...] = jnp.zeros_like(sums)

        @pl.loop(0, PANELS)
        def _(col):
            xv = buf[old, me, col]
            sums[0] += fold(xv * xv)
            sums[1] += fold(xv * x2row[col])

        sum_start(rnd, [t1, sums[0], sums[1]])

    def mix(rnd):
        t1, t2, t3 = sum_finish(rnd, 3)
        cval = (t2 - t3) / (t1 - t2)
        inv = 1.0 / (1.0 - cval)
        for k, val in enumerate(((1.0 - 2.0 * cval) * inv, (1.0 + cval) * inv, inv)):
            coef[k : k + 1, :] = jnp.broadcast_to(val, (1, blk_n))

    def updated(old, col):
        return coef[0:1, :] * buf[old, me, col] + coef[1:2, :] * x2row[col] - coef[2:3, :] * acc[...]

    hx.drain()

    @pl.loop(0, STEPS - 1)
    def _(step):
        old, new = part(step), part(step + 1)
        traces(old, 1 + step)
        ex = Exchange(new, x_place, lambda src: src.x_count)

        @pl.loop(0, SLOTS + 1)
        def _(t):
            at = ex.at(sources[0], t)
            col = at[2]
            acc[...] = product(old, col)

            @pl.when(t == 0)
            def _():
                mix(1 + step)

            buf[new, me, col] = updated(old, col)

            @pl.when(t < sources[0].x_count)
            def _():
                ex.own(at, t, lambda copy: copy.start())

        clear()

        def x_take(masks, first, last):
            for t in range(first, last):
                for mask in masks:
                    src = sources[mask]
                    if t == 4:

                        @pl.when(src.x_count == SLOTS)
                        def _():
                            ex.take(mask, x_at(src, t), t)

                    else:
                        at = x_at(src, t)
                        ex.take(mask, at, t)
                        if (mask, t) in ((XN, 0), (XN + 2, 0), (YN, 1), (YN + 2, 1)):

                            @pl.when(at[2] == me)
                            def _():
                                buf[new, me, at[1]] = buf[new, at[1], at[2]].T

        def x_first(k, at, t):
            src = at[3]
            use_pair(new, at[1], (at[2], x_place(src, 1)[1]))

        def x_second(k, at, t):
            use_diag(new, at[1], at[2])

        def x_last(k, at, t):
            use(new, at[1], at[2])

        near = (PARTNER, XN, YN, XN + 2, YN + 2)
        far = (DIAG, DIAG + 2)
        ex.each((0,), x_first, 0, 1)
        ex.each((0,), x_second, 2, 3)
        ex.each((0,), x_last, 4, 5)
        x_take(near, 0, 2)
        ex.each(near, x_first, 0, 1)
        x_take(near, 2, 4)
        ex.each(near, x_second, 2, 3)
        x_take(near, 4, 5)
        ex.each(near, x_last, 4, 5)
        x_take(far, 0, 2)
        ex.each(far, x_first, 0, 1)
        x_take(far, 2, 4)
        ex.each(far, x_second, 2, 3)
        x_take(far, 4, 5)
        ex.each(far, x_last, 4, 5)
        ex.drain()

    old, end = (STEPS - 1) % 2, STEPS % 2
    traces(old, STEPS)
    sums[2] = jnp.zeros((8, 128), jnp.float32)

    def other(q, mask):
        return 4 * flip(half(q, 4), half(mask, 4)) + 2 * flip(part(half(q)), part(half(mask))) + flip(part(q), part(mask))

    def last_copy(q, mask, to):
        block = buf.at[end, q, other(q, mask)]
        return pltpu.make_async_remote_copy(
            src_ref=block,
            dst_ref=block,
            send_sem=last_send.at[mask],
            recv_sem=last_recv.at[mask],
            device_id=device(to),
            device_id_type=MESH,
        )

    def put(row, b, val):
        out_ref[span(row - 4 * y), span(b)] = val

    def last_mask(d):
        return on * pick(d, (5, 4, 7, 6, 3, 0, 1, 2)) + (1 - on) * pick(d, (0, 2, 4, 5, 6, 7, 1, 3))

    def last_send_to(d):
        return on * pick(d, (4, 1, 6, 1, 2)) + (1 - on)

    def last_sends(d):
        return d < 2 + 3 * on

    @pl.loop(0, PANELS)
    def _(d):
        @pl.when(d < 6 + 2 * on)
        def _():
            mask = last_mask(d)
            col = other(me, mask)
            acc[...] = product(old, col)

            @pl.when(d == 0)
            def _():
                mix(STEPS)

            val = updated(old, col)

            @pl.when(last_sends(d))
            def _():
                buf[end, me, col] = val

            weight = 1 + on * part(mask) * (1 - half(mask, 4))
            sums[2] += fold(val * hrow[col]) * weight.astype(jnp.float32)

            @pl.when(last_sends(d))
            def _():
                last_copy(me, mask, last_send_to(d)).start()

            @pl.when(half(col, 4) == y)
            def _():
                put(col, y, val.T)

            @pl.when(jnp.logical_and(on == 1, mask == 1))
            def _():
                put(me, 1 - y, val)

    sum_start(STEPS + 1, [sums[2]])

    @pl.when(on == 1)
    def _():
        for mask, src in ((3, 2), (0, 1), (2, 1)):
            q = sources[src].q
            last_copy(q, jnp.int32(mask), jnp.int32(src)).wait_recv()
            col = other(q, jnp.int32(mask))
            if mask == 3:
                put(q, 1 - y, buf[end, q, col])
            else:
                put(col, 1 - y, buf[end, q, col].T)

    @pl.when(on == 0)
    def _():
        for mask, src in ((5, 4), (4, 1), (7, 6), (6, 1)):
            q = sources[src].q
            last_copy(q, jnp.int32(mask), jnp.int32(src)).wait_recv()
            col = other(q, jnp.int32(mask))
            if src == YN:
                put(col, 1 - y, buf[end, q, col].T)
            else:
                put(q, 1 - y, buf[end, q, col])

    @pl.loop(0, SLOTS)
    def _(d):
        @pl.when(last_sends(d))
        def _():
            last_copy(me, last_mask(d), last_send_to(d)).wait_send()

    (energy,) = sum_finish(STEPS + 1, 1)
    e_ref[0] = 2.0 * jnp.sum(energy)


def solution(mesh):
    n_cols = mesh.shape["col"]

    def local_fn(ham_blk, bounds, n_occ):
        rows_n, cols_n = ham_blk.shape
        n = cols_n * n_cols
        blk_n = n // PANELS
        f32 = jnp.float32
        return pl.pallas_call(
            lambda *refs: kernel(n, *refs),
            out_shape=(jax.ShapeDtypeStruct((rows_n, cols_n), f32), jax.ShapeDtypeStruct((1,), f32)),
            in_specs=[
                pl.BlockSpec(memory_space=pltpu.SMEM),
                pl.BlockSpec(memory_space=pltpu.SMEM),
                pl.BlockSpec(memory_space=pltpu.HBM),
            ],
            out_specs=(pl.BlockSpec(memory_space=pltpu.VMEM), pl.BlockSpec(memory_space=pltpu.SMEM)),
            scratch_shapes=[
                pltpu.VMEM((rows_n, cols_n), f32),
                pltpu.SemaphoreType.DMA,
                pltpu.VMEM((2, PANELS, PANELS, blk_n, blk_n), f32),
                pltpu.VMEM((PANELS, blk_n, blk_n), f32),
                pltpu.VMEM((PANELS, blk_n, blk_n), f32),
                pltpu.VMEM((blk_n, blk_n), f32),
                pltpu.VMEM((STEPS + 2, PANELS, 8, 128), f32),
                pltpu.VMEM((8, blk_n), f32),
                pltpu.VMEM((3, 8, 128), f32),
                pltpu.SemaphoreType.DMA((PANELS, SLOTS + CORNERS, 3)),
                pltpu.SemaphoreType.DMA((PANELS, SLOTS + CORNERS)),
                pltpu.SemaphoreType.DMA((PANELS,)),
                pltpu.SemaphoreType.DMA((STEPS + 2, PANELS)),
                pltpu.SemaphoreType.DMA((PANELS,)),
                pltpu.SemaphoreType.DMA((PANELS,)),
            ],
            compiler_params=pltpu.CompilerParams(collective_id=0, has_side_effects=True, vmem_limit_bytes=48 << 20),
            name="purify",
        )(bounds, n_occ, ham_blk)

    spec_mat = P(("spin", "row"), "col")
    return jax.shard_map(local_fn, mesh=mesh, in_specs=(spec_mat, P("spin"), P("spin")), out_specs=(spec_mat, P("spin")), check_vma=False)
```

```python
import jax
import jax.numpy as jnp
from jax import lax
from jax.experimental import pallas as pl
from jax.experimental.pallas import tpu as pltpu
from jax.sharding import PartitionSpec as P

STEPS = 3
PANELS = 8
SLOTS = 5
CORNERS = 2
MESH = pl.DeviceIdType.MESH
NN = (((1,), (0,)), ((), ()))
NT = (((1,), (1,)), ((), ()))


def dot(lhs, rhs, dims):
    return lax.dot_general(lhs, rhs, dims, precision=lax.Precision.HIGHEST, preferred_element_type=jnp.float32)


def flag(cond):
    return lax.convert_element_type(cond, jnp.int32)


def pick(index, values):
    return sum(flag(index == k) * v for k, v in enumerate(values) if not (isinstance(v, int) and v == 0))


def half(val, by=2):
    return lax.div(val, jnp.int32(by))


def part(val, by=2):
    return lax.rem(val, jnp.int32(by))


def flip(bit, by):
    return bit + by - 2 * bit * by


def panel_bits(q):
    return q // 4, q % 2, (q // 2) % 2


def packed(digits, base):
    return sum(d * base**k for k, d in enumerate(digits))


def h_blocks(q):
    x, y, c = panel_bits(q)
    if x == y:
        local = {
            (0, 0): ((1, 0), (3, 0), (2, 0), (0, 0), (1, 1)),
            (0, 1): ((3, 0), (1, 0), (1, 1), (2, 0), (3, 1)),
            (1, 0): ((1, 0), (2, 0), (3, 0), (0, 0), (1, 1)),
            (1, 1): ((3, 0), (1, 0), (1, 1), (2, 0), (3, 1)),
        }[x, c]
    else:
        local = tuple((2 * k + (b + y) % 2, b) for b in range(2) for k in range(2))
    return tuple((4 * y + a, 4 * x + 2 * c + b) for a, b in local)


def x_blocks(q):
    x, y, c = panel_bits(q)
    return tuple(q ^ m for m in (4 + 2 * x, 1 + 2 * y, 5 + 2 * y, 0, 2, 7 - 2 * y))


def kernel(n, bounds, n_occ, h_hbm, out_ref, e_ref, h_ref, h_sem, buf, hrow, x2row, acc, parts, coef, sums, send_sem, recv_sem, part_send, part_recv, last_send, last_recv):
    blk_n = n // PANELS
    y = lax.axis_index("row")
    j = lax.axis_index("col")
    x, c = half(j), part(j)
    me = 4 * x + 2 * c + y
    on = 1 - flip(x, y)

    class Source:
        def __init__(self, q, h_pack, h_count, x_pack, x_count):
            self.fields = q, h_pack, h_count, x_pack, x_count
            self.q, self.h_pack, self.h_count, self.x_pack, self.x_count = self.fields

        def __add__(self, other):
            return Source(*(a + b for a, b in zip(self.fields, other.fields)))

        def __mul__(self, by):
            return Source(*(a * by for a in self.fields))

    def device(mask):
        dx, dy, dc = flip(x, half(mask, 4)), flip(y, part(mask)), flip(c, part(half(mask)))
        return (0, dy, 2 * dx + dc)

    def source(mask):
        q = panel(mask)
        return Source(
            q,
            pick(q, [packed([8 * row + col for row, col in h_blocks(k)], 64) for k in range(PANELS)]),
            pick(q, [len(h_blocks(k)) for k in range(PANELS)]),
            pick(q, [packed(x_blocks(k), 8) for k in range(PANELS)]),
            pick(q, [5 - (k // 2) % 2 for k in range(PANELS)]),
        )

    def panel(mask):
        return 4 * flip(x, mask // 4) + 2 * flip(c, (mask // 2) % 2) + flip(y, mask % 2)

    def h_place(src, t):
        code = part(lax.div(src.h_pack, pick(t, [64**k for k in range(SLOTS)])), 64)
        return half(code, 8), part(code, 8)

    def x_place(src, t):
        return src.q, part(lax.div(src.x_pack, pick(t, [8**k for k in range(SLOTS + 1)])), 8)

    def x_at(src, t):
        return src.q, src.q, part(half(src.x_pack, 8**t), 8), src

    devices = [device(jnp.int32(mask)) for mask in range(8)]
    sources = [source(mask) for mask in range(8)]

    PARTNER, XN, YN, DIAG = 2, 4, 1, 5
    FORWARD = {XN: 3, YN: 5, DIAG: 7}

    h_in = pltpu.make_async_copy(h_hbm, h_ref, h_sem)
    h_in.start()

    barrier = pltpu.get_barrier_semaphore()
    for mask in range(1, 8):
        pl.semaphore_signal(barrier, inc=1, device_id=devices[mask], device_id_type=MESH)
    pl.semaphore_wait(barrier, 7)
    h_in.wait()

    class Exchange:
        def __init__(self, buf_id, place, count, own_src=None):
            self.buf_id, self.place, self.count = buf_id, place, count
            self.own_src = own_src or (lambda row, col: buf.at[buf_id, row, col])

        def copy(self, at, t, way, view, src=None, sem=None):
            q, row, col, _ = at
            block = view(buf.at[self.buf_id, row, col])
            return pltpu.make_async_remote_copy(
                src_ref=block if src is None else view(src),
                dst_ref=block,
                send_sem=send_sem.at[way if sem is None else sem, t],
                recv_sem=recv_sem.at[q, t],
                device_id=devices[(PARTNER, XN, YN)[way]],
                device_id_type=MESH,
            )

        def pieces(self, at, t, body):
            mid = blk_n // 2

            @pl.when(at[1] != at[2])
            def _():
                body(t, lambda ref: ref, flag(t == 0) + flag(t == 2))

            @pl.when(at[1] == at[2])
            def _():
                body(t, lambda ref: ref.at[pl.ds(0, mid), :], jnp.int32(0))
                body(t + CORNERS, lambda ref: ref.at[pl.ds(mid, mid), pl.ds(mid, mid)], flag(t == 4))

        def own(self, at, t, act):
            def body(slot, view, x_way):
                for way in range(3):
                    act(self.copy(at, slot, way, view, self.own_src(*at[1:3])))

            self.pieces(at, t, body)

        def forward(self, mask, at, t, act):
            def body(slot, view, x_way):
                act(self.copy(at, slot, 0, view, sem=FORWARD[mask]))
                if mask == XN:

                    @pl.when(x_way == 1)
                    def _():
                        act(self.copy(at, slot, 2, view, sem=FORWARD[mask] + 1))

                if mask == YN:

                    @pl.when(x_way == 0)
                    def _():
                        act(self.copy(at, slot, 1, view, sem=FORWARD[mask] + 1))

            self.pieces(at, t, body)

        def forward_any(self, k, masks, at, t, act):
            for mask in (XN, YN, DIAG):
                if mask in masks:

                    @pl.when(k == masks.index(mask))
                    def _():
                        self.forward(mask, at, t, act)

        def arrive(self, k, masks, at, t):
            self.pieces(at, t, lambda slot, view, x_way: self.copy(at, slot, 0, view).wait_recv())
            self.forward_any(k, masks, at, t, lambda copy: copy.start())
            mid = blk_n // 2

            @pl.when(at[1] == at[2])
            def _():
                block = buf.at[self.buf_id, at[1], at[2]]
                block[mid:, :mid] = block[:mid, mid:].T

        def take(self, mask, at, t):
            mid = blk_n // 2
            views = [(t, lambda ref: ref)]
            if t == 3:
                views = [(t, lambda ref: ref.at[pl.ds(0, mid), :]), (t + CORNERS, lambda ref: ref.at[pl.ds(mid, mid), pl.ds(mid, mid)])]
            for slot, view in views:
                self.copy(at, slot, 0, view).wait_recv()
            for slot, view in views:
                if mask in (XN, YN, DIAG):
                    self.copy(at, slot, 0, view, sem=FORWARD[mask]).start()
                if mask == XN and t in (0, 2):
                    self.copy(at, slot, 2, view, sem=FORWARD[mask] + 1).start()
                if mask == YN and t not in (0, 2):
                    self.copy(at, slot, 1, view, sem=FORWARD[mask] + 1).start()
            if t == 3:
                block = buf.at[self.buf_id, at[1], at[2]]
                block[mid:, :mid] = block[:mid, mid:].T

        def at(self, src, t):
            return (src.q, *self.place(src, t), src)

        def each(self, masks, body, first=0, last=SLOTS):
            srcs = [mask if isinstance(mask, Source) else sources[mask] for mask in masks]
            many = len(srcs)

            @pl.loop(0, (last - first) * many)
            def _(i):
                t, k = first + half(i, many), part(i, many)
                src = srcs[0] if many == 1 else Source(*(pick(k, vals) for vals in zip(*(src.fields for src in srcs))))

                @pl.when(t < self.count(src))
                def _():
                    body(k, self.at(src, t), t)

        def drain(self):
            self.each((0,), lambda k, at, t: self.own(at, t, lambda copy: copy.wait_send()))
            far = (XN, YN, DIAG)
            self.each(far, lambda k, at, t: self.forward_any(k, far, at, t, lambda copy: copy.wait_send()))

    def part_copy(rnd, src, mask):
        rnd = jnp.int32(rnd)
        return pltpu.make_async_remote_copy(
            src_ref=parts.at[rnd, src],
            dst_ref=parts.at[rnd, src],
            send_sem=part_send.at[mask],
            recv_sem=part_recv.at[part(rnd), src],
            device_id=devices[mask],
            device_id_type=MESH,
        )

    def sum_start(rnd, vals):
        for k, val in enumerate(vals):
            parts[rnd, me, k : k + 1] = jnp.sum(val, axis=0, keepdims=True)
        for mask in range(1, 8):
            part_copy(rnd, me, mask).start()

    def sum_finish(rnd, count):
        for mask in range(1, 8):
            part_copy(rnd, sources[mask].q, mask).wait_recv()
        for mask in range(1, 8):
            part_copy(rnd, me, mask).wait_send()
        tot = parts[rnd, 0]
        for q in range(1, PANELS):
            tot = tot + parts[rnd, q]
        return [jnp.sum(tot[k : k + 1], axis=1, keepdims=True) for k in range(count)]

    def fold(val):
        rows, cols = val.shape
        val = jnp.sum(val.reshape(rows // 8, 8, cols), axis=0)
        tot = val[:, :128]
        for k in range(1, cols // 128):
            tot = tot + val[:, k * 128 : (k + 1) * 128]
        return tot

    def span(k):
        return pl.ds(pl.multiple_of(k * blk_n, blk_n), blk_n)

    def clear():
        @pl.loop(0, PANELS)
        def _(col):
            x2row[col] = jnp.zeros((blk_n, blk_n), jnp.float32)

    def h_src(row, col):
        return h_ref.at[span(row - 4 * y), span(col - 2 * j)]

    hx = Exchange(1, h_place, lambda src: src.h_count, h_src)
    hx.each((0,), lambda k, at, t: hx.own(at, t, lambda copy: copy.start()))

    rows_n, cols_n = h_ref.shape
    mu_part = jnp.zeros((8, 128), jnp.float32)
    for k in range(rows_n // blk_n):
        tile = h_ref[k * blk_n : (k + 1) * blk_n, :]
        row_ids = y * rows_n + k * blk_n + lax.broadcasted_iota(jnp.int32, tile.shape, 0)
        col_ids = j * cols_n + lax.broadcasted_iota(jnp.int32, tile.shape, 1)
        mu_part = mu_part + fold(jnp.where(row_ids == col_ids, tile, 0.0))
    sum_start(0, [mu_part])
    clear()

    eye = (lax.broadcasted_iota(jnp.int32, (blk_n, blk_n), 0) == lax.broadcasted_iota(jnp.int32, (blk_n, blk_n), 1)).astype(jnp.float32)
    (trace_h,) = sum_finish(0, 1)
    occ = n_occ[0].astype(jnp.float32)
    mu = trace_h / n
    lam = jnp.minimum(occ / (bounds[1] - mu), (n - occ) / (mu - bounds[0]))
    coef[0:1, :] = jnp.broadcast_to(lam / n, (1, blk_n))
    coef[1:2, :] = jnp.broadcast_to(mu, (1, blk_n))
    coef[2:3, :] = jnp.broadcast_to(jnp.full((1, 1), occ / n, jnp.float32), (1, blk_n))

    def first_x(own, at):
        _, row, col = at[:3]
        blk = h_src(row, col)[...] if own else buf[1, row, col]
        diag = eye * (row == col).astype(jnp.float32)
        val = coef[0:1, :] * (coef[1:2, :] * diag - blk) + coef[2:3, :] * diag
        buf[0, row, col] = val

        @pl.when(row != col)
        def _():
            buf[0, col, row] = val.T

        @pl.when(row == me)
        def _():
            hrow[col] = blk

        @pl.when(jnp.logical_and(col == me, row != me))
        def _():
            hrow[row] = blk.T

    def use(b, row, col):
        blk = buf[b, row, col]
        x2row[col] += dot(buf[b, me, row], blk, NN)
        x2row[row] += dot(buf[b, me, col], blk, NT)
        buf[b, col, row] = blk.T

    def use_pair(b, row, col):
        blk = [buf[b, row, k] for k in col]
        left = buf[b, me, row]
        right = [buf[b, me, k] for k in col]
        for k in range(2):
            x2row[col[k]] += dot(left, blk[k], NN)
        x2row[row] += dot(right[0], blk[0], NT) + dot(right[1], blk[1], NT)
        for k in range(2):
            buf[b, col[k], row] = blk[k].T

    def use_diag(b, row, col):
        blk, mid = buf[b, row, col], buf[b, row, row]
        left = buf[b, me, row]
        right = buf[b, me, col]
        x2row[col] += dot(left, blk, NN)
        x2row[row] += dot(right, blk, NT) + dot(left, mid, NN)
        buf[b, col, row] = blk.T

    def h_take(masks):
        def body(k, at, t):
            hx.arrive(k, masks, at, t)
            first_x(False, at)

        return body

    def h_unit(col, kind):
        cross = half(kind)
        first = 4 * flip(half(col, 4), cross) + (1 - cross) * 2 * kind + cross * flip(part(col), part(kind))
        second = first + 1 + cross
        x2row[col] += dot(buf[0, me, first], buf[0, first, col], NN) + dot(buf[0, me, second], buf[0, second, col], NN)

    @pl.loop(0, 4)
    def _(k):
        first_x(True, (me, 4 * y + k, me))

    hx.each((0,), lambda k, at, t: first_x(True, at))
    hx.each((PARTNER,), h_take((PARTNER,)))

    near = (XN, YN, XN + 2, YN + 2)
    far = (DIAG, DIAG + 2)
    off = 1 - on
    hx.each(near, h_take(near), 0, 1)

    @pl.loop(0, 4 + 4 * on)
    def _(i):
        h_unit(on * (4 * y + half(i)) + off * (4 - 4 * y + i), on * part(i) + off * (2 + y))

    hx.each(near, h_take(near), 1, 3)

    @pl.loop(0, 4 * off)
    def _(i):
        h_unit(4 * y + i, 1 - half(i))

    hx.each(near, h_take(near), 3, SLOTS)

    @pl.loop(0, 16)
    def _(i):
        col, kind = on * (4 * flip(y, half(i, 8)) + half(part(i, 8))) + off * half(i), on * 2 + part(i)

        @pl.when(on + flag(half(col, 4) != y) + flag(kind == half(part(col, 4))) > 0)
        def _():
            h_unit(col, kind)

    @pl.loop(0, 4 * off)
    def _(i):
        h_unit(4 * y + i, 2 + y)

    hx.each(far, h_take(far), 0, 2)

    @pl.loop(0, 4 * off)
    def _(i):
        late_half = half(i)
        h_unit(4 * flip(y, late_half) + 2 * part(i) + late_half * (1 - y), 3 - y)

    hx.each(far, h_take(far), 2, SLOTS)

    @pl.loop(0, 4 + 4 * on)
    def _(i):
        late_half = half(i)
        h_unit(on * (4 - 4 * y + half(i)) + off * (4 * flip(y, late_half) + 2 * part(i) + 1 - late_half * (1 - y)), on * part(i) + off * (3 - y))

    def product(old, col):
        tot = dot(x2row[0], buf[old, 0, col], NN)
        for k in range(1, PANELS):
            tot = tot + dot(x2row[k], buf[old, k, col], NN)
        return tot

    def traces(old, rnd):
        t1 = fold(buf[old, me, me] * eye)
        sums[...] = jnp.zeros_like(sums)

        @pl.loop(0, PANELS)
        def _(col):
            xv = buf[old, me, col]
            sums[0] += fold(xv * xv)
            sums[1] += fold(xv * x2row[col])

        sum_start(rnd, [t1, sums[0], sums[1]])

    def mix(rnd):
        t1, t2, t3 = sum_finish(rnd, 3)
        cval = (t2 - t3) / (t1 - t2)
        inv = 1.0 / (1.0 - cval)
        for k, val in enumerate(((1.0 - 2.0 * cval) * inv, (1.0 + cval) * inv, inv)):
            coef[k : k + 1, :] = jnp.broadcast_to(val, (1, blk_n))

    def updated(old, col):
        return coef[0:1, :] * buf[old, me, col] + coef[1:2, :] * x2row[col] - coef[2:3, :] * acc[...]

    hx.drain()

    @pl.loop(0, STEPS - 1)
    def _(step):
        old, new = part(step), part(step + 1)
        traces(old, 1 + step)
        ex = Exchange(new, x_place, lambda src: src.x_count)

        @pl.loop(0, SLOTS + 1)
        def _(t):
            at = ex.at(sources[0], t)
            col = at[2]
            acc[...] = product(old, col)

            @pl.when(t == 0)
            def _():
                mix(1 + step)

            buf[new, me, col] = updated(old, col)

            @pl.when(t < sources[0].x_count)
            def _():
                ex.own(at, t, lambda copy: copy.start())

        clear()

        def x_take(masks, first, last):
            for t in range(first, last):
                for mask in masks:
                    src = sources[mask]
                    if t == 4:

                        @pl.when(src.x_count == SLOTS)
                        def _():
                            ex.take(mask, x_at(src, t), t)

                    else:
                        at = x_at(src, t)
                        ex.take(mask, at, t)
                        if (mask, t) in ((XN, 0), (XN + 2, 0), (YN, 1), (YN + 2, 1)):

                            @pl.when(at[2] == me)
                            def _():
                                buf[new, me, at[1]] = buf[new, at[1], at[2]].T

        def x_first(k, at, t):
            src = at[3]
            use_pair(new, at[1], (at[2], x_place(src, 1)[1]))

        def x_second(k, at, t):
            use_diag(new, at[1], at[2])

        def x_last(k, at, t):
            use(new, at[1], at[2])

        near = (PARTNER, XN, YN, XN + 2, YN + 2)
        far = (DIAG, DIAG + 2)
        ex.each((0,), x_first, 0, 1)
        ex.each((0,), x_second, 2, 3)
        ex.each((0,), x_last, 4, 5)
        x_take(near, 0, 2)
        ex.each(near, x_first, 0, 1)
        x_take(near, 2, 4)
        ex.each(near, x_second, 2, 3)
        x_take(near, 4, 5)
        ex.each(near, x_last, 4, 5)
        x_take(far, 0, 2)
        ex.each(far, x_first, 0, 1)
        x_take(far, 2, 4)
        ex.each(far, x_second, 2, 3)
        x_take(far, 4, 5)
        ex.each(far, x_last, 4, 5)
        ex.drain()

    old, end = (STEPS - 1) % 2, STEPS % 2
    traces(old, STEPS)
    sums[2] = jnp.zeros((8, 128), jnp.float32)

    def other(q, mask):
        return 4 * flip(half(q, 4), half(mask, 4)) + 2 * flip(part(half(q)), part(half(mask))) + flip(part(q), part(mask))

    def last_copy(q, mask, to):
        block = buf.at[end, q, other(q, mask)]
        return pltpu.make_async_remote_copy(
            src_ref=block,
            dst_ref=block,
            send_sem=last_send.at[mask],
            recv_sem=last_recv.at[mask],
            device_id=device(to),
            device_id_type=MESH,
        )

    def put(row, b, val):
        out_ref[span(row - 4 * y), span(b)] = val

    def last_mask(d):
        return on * pick(d, (5, 4, 7, 6, 3, 0, 1, 2)) + (1 - on) * pick(d, (0, 2, 4, 5, 6, 7, 1, 3))

    def last_send_to(d):
        return on * pick(d, (4, 1, 6, 1, 2)) + (1 - on)

    def last_sends(d):
        return d < 2 + 3 * on

    @pl.loop(0, PANELS)
    def _(d):
        @pl.when(d < 6 + 2 * on)
        def _():
            mask = last_mask(d)
            col = other(me, mask)
            acc[...] = product(old, col)

            @pl.when(d == 0)
            def _():
                mix(STEPS)

            val = updated(old, col)

            @pl.when(last_sends(d))
            def _():
                buf[end, me, col] = val

            weight = 1 + on * part(mask) * (1 - half(mask, 4))
            sums[2] += fold(val * hrow[col]) * weight.astype(jnp.float32)

            @pl.when(last_sends(d))
            def _():
                last_copy(me, mask, last_send_to(d)).start()

            @pl.when(half(col, 4) == y)
            def _():
                put(col, y, val.T)

            @pl.when(jnp.logical_and(on == 1, mask == 1))
            def _():
                put(me, 1 - y, val)

    sum_start(STEPS + 1, [sums[2]])

    @pl.when(on == 1)
    def _():
        for mask, src in ((3, 2), (0, 1), (2, 1)):
            q = sources[src].q
            last_copy(q, jnp.int32(mask), jnp.int32(src)).wait_recv()
            col = other(q, jnp.int32(mask))
            if mask == 3:
                put(q, 1 - y, buf[end, q, col])
            else:
                put(col, 1 - y, buf[end, q, col].T)

    @pl.when(on == 0)
    def _():
        for mask, src in ((5, 4), (4, 1), (7, 6), (6, 1)):
            q = sources[src].q
            last_copy(q, jnp.int32(mask), jnp.int32(src)).wait_recv()
            col = other(q, jnp.int32(mask))
            if src == YN:
                put(col, 1 - y, buf[end, q, col].T)
            else:
                put(q, 1 - y, buf[end, q, col])

    @pl.loop(0, SLOTS)
    def _(d):
        @pl.when(last_sends(d))
        def _():
            last_copy(me, last_mask(d), last_send_to(d)).wait_send()

    (energy,) = sum_finish(STEPS + 1, 1)
    e_ref[0] = 2.0 * jnp.sum(energy)


def solution(mesh):
    n_cols = mesh.shape["col"]

    def local_fn(ham_blk, bounds, n_occ):
        rows_n, cols_n = ham_blk.shape
        n = cols_n * n_cols
        blk_n = n // PANELS
        f32 = jnp.float32
        return pl.pallas_call(
            lambda *refs: kernel(n, *refs),
            out_shape=(jax.ShapeDtypeStruct((rows_n, cols_n), f32), jax.ShapeDtypeStruct((1,), f32)),
            in_specs=[
                pl.BlockSpec(memory_space=pltpu.SMEM),
                pl.BlockSpec(memory_space=pltpu.SMEM),
                pl.BlockSpec(memory_space=pltpu.HBM),
            ],
            out_specs=(pl.BlockSpec(memory_space=pltpu.VMEM), pl.BlockSpec(memory_space=pltpu.SMEM)),
            scratch_shapes=[
                pltpu.VMEM((rows_n, cols_n), f32),
                pltpu.SemaphoreType.DMA,
                pltpu.VMEM((2, PANELS, PANELS, blk_n, blk_n), f32),
                pltpu.VMEM((PANELS, blk_n, blk_n), f32),
                pltpu.VMEM((PANELS, blk_n, blk_n), f32),
                pltpu.VMEM((blk_n, blk_n), f32),
                pltpu.VMEM((STEPS + 2, PANELS, 8, 128), f32),
                pltpu.VMEM((8, blk_n), f32),
                pltpu.VMEM((3, 8, 128), f32),
                pltpu.SemaphoreType.DMA((8, SLOTS + CORNERS)),
                pltpu.SemaphoreType.DMA((PANELS, SLOTS + CORNERS)),
                pltpu.SemaphoreType.DMA((PANELS,)),
                pltpu.SemaphoreType.DMA((2, PANELS)),
                pltpu.SemaphoreType.DMA((PANELS,)),
                pltpu.SemaphoreType.DMA((PANELS,)),
            ],
            compiler_params=pltpu.CompilerParams(collective_id=0, has_side_effects=True, vmem_limit_bytes=48 << 20),
            name="purify",
        )(bounds, n_occ, ham_blk)

    spec_mat = P(("spin", "row"), "col")
    return jax.shard_map(local_fn, mesh=mesh, in_specs=(spec_mat, P("spin"), P("spin")), out_specs=(spec_mat, P("spin")), check_vma=False)
```
